512 devices in a mesh: grp: 64 (over z, x), head: 8 (over y, core).
Axes of the slice: x: 4, y: 4, z: 16, core: 2. Of those that a mesh axis runs over, the one named last changes fastest.
Arguments:
- residual: bfloat16 [1024, 2880], P('grp'), may hold values from -4 to 4
- queries: bfloat16 [1024, 8, 256], P('grp', 'head'), may hold values from -200 to 200
- kv_cache: bfloat16 [1024, 8, 128, 128], P('grp', 'head'), may hold values from -5 to 5
- new_kv: bfloat16 [1024, 8, 128], P('grp', 'head'), may hold values from -5 to 5
- positions: int32 [1024], P('grp'), may hold values from 0 to 383
- sink_logits: float32 [8, 4], P('head'), may hold values from 0 to 5
- out_proj: bfloat16 [8, 256, 2880], P('head'), may hold values from -0.375 to 0.375
- norm_gain: float32 [2880], replicated, may hold values from 0.5 to 1.5
- route_ids: int32 [1024, 4], P('grp'), may hold values from 0 to 63, all different within a row; in each aligned block of 16 rows (0 to 15, 16 to 31, ...) at most 2 rows name the same one
- route_weights: int32 [1024, 4], P('grp'), may hold values from 1 to 65535
- w_gate_up: bfloat16 [64, 2880, 2880], P('grp', None, 'head'), may hold values from -0.109375 to 0.109375
- w_down: bfloat16 [64, 1440, 2880], P('grp', 'head'), may hold values from -0.15625 to 0.15625
Outputs:
- layer_out: bfloat16 [1024, 2880], P('grp', 'head')
The draws below stay inside these ranges and needn't reach their ends.
Inputs may be any that keep to these rules, and one draw needn't show every extreme that they name: `route_ids`: in the 16 rows of one index of grp, at most 2 rows name the same expert; each row names 4 different experts.
All inputs are finite; a program needn't handle non-finite values.
Results may differ from the reference program's by a relative error of at most 0.025.
Values may be sent and summed in bfloat16 or wider, within the bound.
No kernel may reach another device: no remote copies, remote signals or barrier semaphores. Data moves between devices by JAX's collectives and lax.ppermute only.
A program may use at most 64 MiB of HBM per device.

```python
import math
import jax
import jax.numpy as jnp
import numpy as np
from jax import lax

D = 2880
HD = 64
KVH = 8
GQ = 4
WIN = 128
FFE = 1440
TOPK = 4
REQ_DEV = 16
CAP = 2
TOKENS = 1024
EXPERTS = 64
N_GRP = 64


def attention_inputs(key):
    key_pos = jax.random.fold_in(key, 11)
    key_cycle = jax.random.fold_in(key, 12)
    key_query = jax.random.fold_in(key, 13)
    positions = jax.random.randint(key_pos, (TOKENS,), 0, 3 * WIN).astype(jnp.int32)
    positions = positions.at[0].set(3 * WIN - 1).at[1].set(0)
    cycle_cache = jax.random.truncated_normal(key_cycle, -5.0, 5.0, (TOKENS, KVH, WIN, 2 * HD), jnp.float32)
    queries = jax.random.truncated_normal(key_query, -5.0, 5.0, (TOKENS, KVH, GQ * HD), jnp.float32)
    return (positions, cycle_cache, queries)


def draw_positions(key, part):
    return attention_inputs(key)[0]


def draw_kv_cache(key, part):
    return attention_inputs(key)[1].astype(jnp.bfloat16)


def draw_queries(key, part):
    return attention_inputs(key)[2].astype(jnp.bfloat16)


def place_ends(entries, rng, low, top_value):
    extent = entries.shape
    index_at = [jax.random.randint(jax.random.fold_in(rng, axis), (), 0, extent[axis]) for axis in range(len(extent))]
    entries = entries.at[tuple(index_at)].set(low)
    longest = extent.index(max(extent))
    index_at[longest] = (index_at[longest] + 1) % extent[longest]
    return entries.at[tuple(index_at)].set(top_value)


def levels(key, dims, pieces, low, high):
    level, own = 1.0, jax.random.fold_in(key, 6)
    for axis_at, shards_of in pieces:
        draws = jnp.exp(jax.random.uniform(jax.random.fold_in(own, axis_at), (shards_of,), jnp.float32, low / len(pieces), high / len(pieces)))
        level = level * jnp.repeat(draws, dims[axis_at] // shards_of).reshape([-1 if axis == axis_at else 1 for axis in range(len(dims))])
    return level


def deal_out(key, own, number, rows, number_of, top, most, skew):
    ranking = jax.random.permutation(key, number_of)
    crowded, ordinary = load_shares(number_of, rows * top, most, skew, True), load_shares(number_of, rows * top, most, skew, False)
    places = jnp.arange(number_of)

    def named(tallies, offset_by):
        used = int((tallies > 0).sum())
        fixed = max(1, used // 4)
        passed = fixed + (places - fixed + offset_by * (used - fixed)) % max(1, number_of - fixed)
        return jnp.zeros((number_of,), jnp.int32).at[ranking[jnp.where(places < fixed, places, passed)]].set(jnp.asarray(tallies, jnp.int32))

    tallies = jnp.where(number % 4 == 0, named(crowded, number // 4), named(ordinary, number - number // 4 - 1))
    mixed = jax.random.permutation(jax.random.fold_in(own, 3), number_of)
    giver, taker = mixed[0:number_of // 2 * 2:2], mixed[1:number_of // 2 * 2:2]
    room = jnp.minimum(tallies[giver] - 1, most - tallies[taker]) // 2
    room = jnp.where((giver == ranking[0]) | (taker == ranking[0]) | (tallies[taker] == 0), 0, jnp.maximum(room, 0))
    passed = jax.random.randint(jax.random.fold_in(own, 4), (number_of // 2,), 0, 1 << 20) % (room + 1)
    tallies = tallies.at[giver].add(-passed).at[taker].add(passed)
    items = jnp.searchsorted(jnp.cumsum(tallies), jnp.arange(rows * top), side="right").astype(jnp.int32)
    table = items.reshape(top, rows).T
    table = table[jax.random.permutation(jax.random.fold_in(own, 1), rows)]
    offset_by = jax.random.randint(jax.random.fold_in(own, 2), (rows, 1), 0, top)
    return jnp.take_along_axis(table, (jnp.arange(top)[None, :] + offset_by) % top, axis=1)


def load_shares(amount, total, most, slope, full):
    loads = [(1 << 20) // math.isqrt(standing ** slope) + 1 for standing in range(1, amount + 1)]
    largest = most if full else min(most, max(-(-total // amount), total * loads[0] // sum(loads)))
    least = 1 if total - largest >= amount - 1 else 0
    given, surplus = [largest] + [least] * (amount - 1), total - largest - least * (amount - 1)
    while surplus > 0:
        candidates = [i for i in range(1, amount) if given[i] < largest] or [i for i in range(1, amount) if given[i] < most]
        mass, budget = sum([loads[i] for i in candidates]), surplus
        for i in candidates:
            more = min(most - given[i], max(1, budget * loads[i] // mass), surplus)
            given[i] = given[i] + more
            surplus = surplus - more
    return np.array(given)


def noise(key, shape, deviation, reach, pieces=(), kind=jnp.bfloat16):
    level = levels(key, shape, pieces, -0.22, 0.18) if pieces else 1.0
    array = jax.random.normal(key, shape, jnp.float32) * deviation * level
    return jnp.minimum(jnp.maximum(array, -reach), reach).astype(kind)


def setup_inputs(seed: int = 0) -> dict:
    streams_of = jax.random.split(jax.random.key(seed), 13)
    residual = noise(streams_of[0], (TOKENS, D), 0.5, 4.0, ((0, 64),))
    queries = draw_queries(jax.random.fold_in(streams_of[12], 71), 0)
    kv_cache = draw_kv_cache(jax.random.fold_in(streams_of[12], 71), 0)
    new_kv = noise(streams_of[3], (TOKENS, KVH, 2 * HD), 1.0, 5.0, ((0, 64), (1, 8)))
    positions = draw_positions(jax.random.fold_in(streams_of[12], 71), 0)
    sink_logits = jnp.clip(5.0 * jax.random.uniform(streams_of[5], (KVH, GQ), jnp.float32) ** levels(streams_of[5], (KVH, GQ), ((0, 8),), -0.2, 0.2), 0.0, 5.0)
    out_proj = noise(streams_of[6], (KVH, GQ * HD, D), (GQ * HD) ** -0.5, 0.375, ((0, 8),))
    norm_gain = jnp.clip(1.0 + 0.1 * jax.random.normal(streams_of[7], (D,), jnp.float32), 0.5, 1.5)
    route_ids_keys = jax.random.split(jax.random.fold_in(streams_of[8], 1), TOKENS // REQ_DEV)
    route_ids_turns = jax.random.permutation(jax.random.fold_in(streams_of[8], 3), TOKENS // REQ_DEV)
    route_ids = jax.vmap(lambda own, number: deal_out(jax.random.fold_in(streams_of[8], 2), own, number, REQ_DEV, EXPERTS, TOPK, CAP, 2))(route_ids_keys, route_ids_turns).reshape((TOKENS, TOPK))
    route_weights = place_ends(jax.random.randint(streams_of[9], (TOKENS, TOPK), 1, 65536), jax.random.fold_in(streams_of[9], 1), 1, 65535).astype(jnp.int32)
    w_gate_up = noise(streams_of[10], (EXPERTS, D, 2 * FFE), D ** -0.5, 0.109375, ((0, 64), (2, 8)))
    w_down = noise(streams_of[11], (EXPERTS, FFE, D), FFE ** -0.5, 0.15625, ((0, 64), (1, 8)))
    return {"residual": residual, "queries": queries, "kv_cache": kv_cache, "new_kv": new_kv, "positions": positions, "sink_logits": sink_logits, "out_proj": out_proj, "norm_gain": norm_gain, "route_ids": route_ids, "route_weights": route_weights, "w_gate_up": w_gate_up, "w_down": w_down}


epsilon = 1e-05
swish_alpha = 1.702

def rms_norm(values, gain):
    as_float = values.astype(jnp.float32)
    mean_square = lax.optimization_barrier(jnp.mean(as_float * as_float, axis=-1, keepdims=True))
    return (as_float * lax.rsqrt(mean_square + epsilon) * gain).astype(jnp.bfloat16)

def expert_apply(inputs):
    buffer_rows, gate_up, down_weight = inputs
    projected = jnp.dot(buffer_rows, gate_up, preferred_element_type=jnp.float32)
    pairs_view = projected.reshape(projected.shape[0], -1, 2)
    gate_half = pairs_view[..., 0]
    up_half = pairs_view[..., 1]
    activated = ((up_half + 1.0) * gate_half * jax.nn.sigmoid(swish_alpha * gate_half)).astype(jnp.bfloat16)
    return jnp.dot(activated, down_weight, preferred_element_type=jnp.float32)

def reference(residual, queries, kv_cache, new_kv, positions, sink_logits, out_proj, norm_gain, route_ids, route_weights, w_gate_up, w_down):
    slot_iota = jnp.arange(WIN, dtype=jnp.int32)
    current = positions % WIN
    slot_lag = (positions[:, None] - slot_iota[None, :]) % WIN
    is_valid = slot_lag <= positions[:, None]
    is_new = slot_iota[None, :] == current[:, None]
    merged = jnp.where(is_new[:, None, :, None], new_kv[:, :, None, :], kv_cache)
    key_part = merged[..., :HD].astype(jnp.float32)
    value_part = merged[..., HD:].astype(jnp.float32)
    query_part = queries.reshape(TOKENS, KVH, GQ, HD).astype(jnp.float32)
    scores = jnp.einsum('thgd,thwd->thgw', query_part, key_part) * HD ** (-0.5)
    scores = jnp.where(is_valid[:, None, None, :], scores, -jnp.inf)
    sink_col = sink_logits[None, :, :, None]
    largest = jnp.maximum(lax.optimization_barrier(jnp.max(scores, axis=-1, keepdims=True)), sink_col)
    weights_exp = jnp.exp(scores - largest)
    denominator = lax.optimization_barrier(jnp.sum(weights_exp, axis=-1, keepdims=True)) + jnp.exp(sink_col - largest)
    weights = (weights_exp / denominator).astype(jnp.bfloat16)
    mixed = jnp.einsum('thgw,thwd->thgd', weights.astype(jnp.float32), value_part).astype(jnp.bfloat16)
    attention = jnp.dot(mixed.reshape(TOKENS, KVH * GQ * HD), out_proj.reshape(KVH * GQ * HD, D), preferred_element_type=jnp.float32)
    hidden = (residual.astype(jnp.float32) + attention).astype(jnp.bfloat16)
    normed = rms_norm(hidden, norm_gain)
    per_block = REQ_DEV * TOPK
    grouped_ids = route_ids.reshape(N_GRP, per_block).astype(jnp.int32)
    assign_iota = jnp.arange(per_block, dtype=jnp.int32)
    earlier = (grouped_ids[:, :, None] == grouped_ids[:, None, :]) & (assign_iota[:, None] > assign_iota[None, :])
    slot_rank = lax.optimization_barrier(jnp.sum(earlier.astype(jnp.int32), axis=-1)).astype(jnp.int32)
    block_iota = jnp.arange(N_GRP, dtype=jnp.int32)[:, None]
    slot_index = (grouped_ids * (N_GRP * CAP) + block_iota * CAP + slot_rank).reshape(-1).astype(jnp.int32)
    total_slots = EXPERTS * N_GRP * CAP
    source_row = jnp.zeros((total_slots,), jnp.int32).at[slot_index].set((jnp.arange(TOKENS * TOPK, dtype=jnp.int32) // TOPK).astype(jnp.int32))
    filled = jnp.zeros((total_slots,), jnp.bool_).at[slot_index].set(True)
    buffers = jnp.where(filled[:, None], normed[source_row], jnp.zeros((), jnp.bfloat16)).reshape(EXPERTS, N_GRP * CAP, D)
    expert_outs = lax.map(expert_apply, (buffers, w_gate_up, w_down))
    picked = expert_outs.reshape(total_slots, D)[slot_index]
    weight_vec = route_weights.reshape(-1).astype(jnp.float32) / 65536.0
    mixture = lax.optimization_barrier(jnp.sum((picked * weight_vec[:, None]).reshape(TOKENS, TOPK, D), axis=1))
    return (hidden.astype(jnp.float32) + mixture).astype(jnp.bfloat16)
```

```python
import functools

import jax
import jax.numpy as jnp
from jax import lax
from jax.experimental import pallas as pl
from jax.experimental.pallas import tpu as pltpu
from jax.sharding import Mesh, PartitionSpec as P

epsilon = 1e-05
swish_alpha = 1.702

GRID = (16, 4, 4, 2)
GRP = ("z", "x")
HEAD = ("y", "core")
MIB = 1 << 20
KV_PIECES = 4


def attend_kernel(
    pos_hbm,
    sink_hbm,
    q_hbm,
    kv_hbm,
    new_hbm,
    proj_hbm,
    out_ref,
    pos_ref,
    sink_ref,
    q_ref,
    kv_ref,
    new_ref,
    proj_ref,
    sems,
):
    rows, window, width = kv_ref.shape
    piece = rows // KV_PIECES
    copies = [
        pltpu.make_async_copy(src, dst, sems.at[i])
        for i, (src, dst) in enumerate(
            [(q_hbm, q_ref), (new_hbm, new_ref), (pos_hbm, pos_ref), (sink_hbm, sink_ref)]
        )
    ]
    kv_copies = [
        pltpu.make_async_copy(
            kv_hbm.at[pl.ds(i * piece, piece)], kv_ref.at[pl.ds(i * piece, piece)], sems.at[4 + i]
        )
        for i in range(KV_PIECES)
    ]
    proj_copy = pltpu.make_async_copy(proj_hbm, proj_ref, sems.at[4 + KV_PIECES])
    for copy in copies + kv_copies:
        copy.start()
    proj_copy.start()
    for copy in copies:
        copy.wait()
    half = width // 2
    groups = 4
    shares, _, share_width = out_ref.shape
    lane = lax.broadcasted_iota(jnp.int32, (rows, width), 1)
    row = lax.broadcasted_iota(jnp.int32, (rows, width), 0)
    low = lane < half
    q = q_ref[...].astype(jnp.float32)
    parts = []
    for pair in range(groups // 2):
        both = q[:, pair * width : (pair + 1) * width]
        parts.append(jnp.where(low, both, 0.0))
        parts.append(jnp.where(low, pltpu.roll(both, half, 1), 0.0))
    stacked = jnp.concatenate(parts, axis=0)
    stacked_low = stacked.astype(jnp.bfloat16)
    new = new_ref[...].astype(jnp.float32)
    new_all = jnp.concatenate([new] * groups, axis=0)

    pos = jnp.zeros((rows, width), jnp.int32)
    for t in range(rows):
        pos = jnp.where(row == t, pos_ref[t], pos)
    pos = jnp.concatenate([pos] * groups, axis=0)
    lanes = lax.broadcasted_iota(jnp.int32, pos.shape, 1)
    request = lax.broadcasted_iota(jnp.int32, pos.shape, 0) % rows
    group = lax.broadcasted_iota(jnp.int32, (groups * rows, 1), 0) // rows
    sink = jnp.zeros((groups * rows, 1), jnp.float32)
    for g in range(groups):
        sink = jnp.where(group == g, sink_ref[0, g], sink)

    scores = jnp.zeros((groups * rows, window), jnp.float32)
    for t in range(rows):
        if t % piece == 0:
            kv_copies[t // piece].wait()
        found = lax.dot_general(
            stacked_low, kv_ref[t], (((1,), (1,)), ((), ())), preferred_element_type=jnp.float32
        )
        scores = jnp.where(request == t, found, scores)
    newest = jnp.sum(stacked * new_all, axis=1, keepdims=True)
    is_new = lanes == (pos & (window - 1))
    scores = jnp.where(is_new, newest, scores) * (half**-0.5)
    scores = jnp.where(lanes <= pos, scores, -jnp.inf)
    largest = jnp.maximum(jnp.max(scores, axis=1, keepdims=True), sink)
    raised = jnp.exp(scores - largest)
    total = jnp.sum(raised, axis=1, keepdims=True) + jnp.exp(sink - largest)
    weights = (raised / total).astype(jnp.bfloat16).astype(jnp.float32)
    newest_weight = jnp.sum(jnp.where(is_new, weights, 0.0), axis=1, keepdims=True)
    older = jnp.where(is_new, 0.0, weights).astype(jnp.bfloat16)
    mixed = jnp.zeros((groups * rows, width), jnp.float32)
    for t in range(rows):
        found = jnp.dot(older, kv_ref[t], preferred_element_type=jnp.float32)
        mixed = jnp.where(request == t, found, mixed)
    mixed = mixed + newest_weight * new_all
    merged = []
    for pair in range(groups // 2):
        first = mixed[2 * pair * rows : (2 * pair + 1) * rows]
        second = mixed[(2 * pair + 1) * rows : (2 * pair + 2) * rows]
        merged.append(jnp.where(low, pltpu.roll(first, half, 1), second))
    merged = jnp.concatenate(merged, axis=1).astype(jnp.bfloat16)
    proj_copy.wait()
    for s in range(shares):
        out_ref[s] = lax.dot_general(
            merged,
            proj_ref[pl.ds(s * share_width, share_width), :],
            (((1,), (1,)), ((), ())),
            preferred_element_type=jnp.float32,
        ).astype(jnp.bfloat16)


def attend(positions, sink_logits, queries, kv_cache, new_kv, out_proj):
    rows, _, window, width = kv_cache.shape
    features = out_proj.shape[2]
    hbm = pl.BlockSpec(memory_space=pltpu.HBM)
    return pl.pallas_call(
        attend_kernel,
        out_shape=jax.ShapeDtypeStruct((8, rows, features // 8), jnp.bfloat16),
        in_specs=[hbm] * 6,
        out_specs=pl.BlockSpec(memory_space=pltpu.VMEM),
        scratch_shapes=[
            pltpu.SMEM((rows,), jnp.int32),
            pltpu.SMEM(sink_logits.shape, jnp.float32),
            pltpu.VMEM((rows, queries.shape[2]), jnp.bfloat16),
            pltpu.VMEM((rows, window, width), jnp.bfloat16),
            pltpu.VMEM((rows, width), jnp.bfloat16),
            pltpu.VMEM((features, out_proj.shape[1]), jnp.bfloat16),
            pltpu.SemaphoreType.DMA((5 + KV_PIECES,)),
        ],
        compiler_params=pltpu.CompilerParams(vmem_limit_bytes=8 * MIB),
        name="attend",
    )(
        *(
            pltpu.with_memory_space_constraint(x, pltpu.HBM)
            for x in (
                positions,
                sink_logits,
                queries.reshape(rows, -1),
                kv_cache.reshape(rows, window, width),
                new_kv.reshape(rows, width),
                jnp.swapaxes(out_proj[0], 0, 1),
            )
        )
    )


def up_kernel(core_ref, x_ref, w_ref, down_ref, act_ref, send_ref, held_ref):
    other = 1 - core_ref[0]
    x = x_ref[...]
    wide = x.astype(jnp.float32)
    mean_square = jnp.mean(wide * wide, axis=0, keepdims=True)
    projected = jnp.dot(w_ref[...], x, preferred_element_type=jnp.float32)
    held_ref[...] = projected * lax.rsqrt(mean_square + epsilon)
    hidden_units = held_ref.shape[0] // 2
    gate = held_ref[pl.ds(0, hidden_units, stride=2), :]
    up = held_ref[pl.ds(1, hidden_units, stride=2), :]
    act = ((up + 1.0) * gate * jax.nn.sigmoid(swish_alpha * gate)).astype(jnp.bfloat16)
    act_ref[...] = act
    send_ref[...] = jnp.dot(
        down_ref[other], act, preferred_element_type=jnp.float32
    ).astype(jnp.bfloat16)


def down_kernel(core_ref, act_ref, down_ref, out_ref):
    out_ref[...] = jnp.dot(
        down_ref[core_ref[0]], act_ref[...], preferred_element_type=jnp.float32
    )


def local(
    residual,
    queries,
    kv_cache,
    new_kv,
    positions,
    sink_logits,
    out_proj,
    norm_gain,
    route_ids,
    route_weights,
    w_gate_up,
    w_down,
):
    rows, features = residual.shape
    experts = lax.axis_size(GRP)
    shares = lax.axis_size(HEAD)
    y_size = lax.axis_size("y")
    share = features // shares
    topk = route_ids.shape[1]
    capacity = 2
    slots = experts * capacity
    units = w_down.shape[1]
    core = lax.axis_index("core").astype(jnp.int32).reshape(1)
    vmem = pl.BlockSpec(memory_space=pltpu.VMEM)
    smem = pl.BlockSpec(memory_space=pltpu.SMEM)

    parts = attend(positions, sink_logits, queries, kv_cache, new_kv, out_proj)
    parts = lax.all_to_all(parts, HEAD, 0, 0, tiled=True)
    attention = jnp.sum(parts.astype(jnp.float32), axis=0)
    resid_here = lax.optimization_barrier(
        lax.dynamic_slice_in_dim(residual, lax.axis_index(HEAD) * share, share, 1)
    )
    hidden = (resid_here.astype(jnp.float32) + attention).astype(jnp.bfloat16)

    flat_ids = route_ids.reshape(-1)
    order = jnp.arange(rows * topk, dtype=jnp.int32)
    earlier = (flat_ids[:, None] == flat_ids[None, :]) & (order[:, None] > order[None, :])
    slot = (flat_ids * capacity + jnp.sum(earlier.astype(jnp.int32), axis=1)).reshape(rows, topk)
    hit = slot[:, :, None] == jnp.arange(slots, dtype=jnp.int32)[None, None, :]
    scale = route_weights.astype(jnp.float32) / 65536.0
    pick, combine = lax.optimization_barrier(
        (
            jnp.sum(hit.astype(jnp.float32), axis=1).astype(jnp.bfloat16),
            jnp.sum(jnp.where(hit, scale[:, :, None], 0.0), axis=1),
        )
    )

    gate_up = (
        jnp.swapaxes(w_gate_up[0], 0, 1).astype(jnp.float32) * norm_gain[None, :]
    ).astype(jnp.bfloat16)
    down = (
        w_down[0].reshape(units, y_size, 2, share).transpose(2, 1, 3, 0).reshape(2, -1, units)
    )

    outgoing = lax.dot_general(
        pick, hidden, (((0,), (0,)), ((), ())), preferred_element_type=jnp.float32
    ).astype(jnp.bfloat16)
    got = lax.all_to_all(outgoing.reshape(experts, capacity, share), GRP, 0, 0, tiled=True)
    got, gate_up, down = lax.optimization_barrier((got, gate_up, down))
    got = jnp.swapaxes(got.reshape(slots, share), 0, 1)
    mine = lax.all_to_all(
        jnp.broadcast_to(got[None], (y_size, share, slots)), "y", 0, 0, tiled=True
    )
    swap = [(0, 1), (1, 0)]
    theirs = lax.ppermute(mine, "core", swap)
    is_low = core[0] == 0
    full = jnp.stack(
        [jnp.where(is_low, mine, theirs), jnp.where(is_low, theirs, mine)], axis=1
    ).reshape(features, slots)

    act, sent = pl.pallas_call(
        up_kernel,
        out_shape=(
            jax.ShapeDtypeStruct((units, slots), jnp.bfloat16),
            jax.ShapeDtypeStruct((y_size * share, slots), jnp.bfloat16),
        ),
        in_specs=[smem, vmem, vmem, vmem],
        out_specs=(vmem, vmem),
        scratch_shapes=[pltpu.VMEM((2 * units, slots), jnp.float32)],
        compiler_params=pltpu.CompilerParams(vmem_limit_bytes=12 * MIB),
        name="up",
    )(core, full, gate_up, down)
    arrived = lax.ppermute(sent, "core", swap)
    own = pl.pallas_call(
        down_kernel,
        out_shape=jax.ShapeDtypeStruct((y_size * share, slots), jnp.float32),
        in_specs=[smem, vmem, vmem],
        out_specs=vmem,
        compiler_params=pltpu.CompilerParams(vmem_limit_bytes=12 * MIB),
        name="down",
    )(core, act, down)
    paired = (own + arrived.astype(jnp.float32)).astype(jnp.bfloat16)
    paired = lax.all_to_all(paired.reshape(y_size, share, slots), "y", 0, 0, tiled=True)
    summed = jnp.sum(paired.astype(jnp.float32), axis=0).astype(jnp.bfloat16)
    back = lax.all_to_all(
        jnp.swapaxes(summed, 0, 1).reshape(experts, capacity, share), GRP, 0, 0, tiled=True
    )
    mixture = jnp.dot(
        combine,
        back.reshape(slots, share).astype(jnp.float32),
        precision=lax.Precision.HIGHEST,
    )
    return (hidden.astype(jnp.float32) + mixture).astype(jnp.bfloat16)


def solution(mesh):
    fine = Mesh(mesh.devices.reshape(GRID), ("z", "x", "y", "core"))
    in_specs = (
        P(GRP, None),
        P(GRP, HEAD, None),
        P(GRP, HEAD, None, None),
        P(GRP, HEAD, None),
        P(GRP),
        P(HEAD, None),
        P(HEAD, None, None),
        P(),
        P(GRP, None),
        P(GRP, None),
        P(GRP, None, HEAD),
        P(GRP, HEAD, None),
    )
    return jax.shard_map(
        local, mesh=fine, in_specs=in_specs, out_specs=P(GRP, HEAD), check_vma=False
    )
```

```python
import jax
import jax.numpy as jnp
from jax import lax
from jax.experimental import pallas as pl
from jax.experimental.pallas import tpu as pltpu
from jax.sharding import Mesh, PartitionSpec as P

epsilon = 1e-05
swish_alpha = 1.702

GRID = (16, 4, 4, 2)
GRP = ("z", "x")
HEAD = ("y", "core")
MIB = 1 << 20
KV_PIECES = 4


def attend_kernel(
    pos_hbm,
    sink_hbm,
    q_hbm,
    kv_hbm,
    new_hbm,
    proj_hbm,
    ids_hbm,
    scale_hbm,
    resid_hbm,
    out_ref,
    pick_ref,
    combine_ref,
    share_ref,
    pos_ref,
    sink_ref,
    q_ref,
    kv_ref,
    new_ref,
    proj_ref,
    ids_ref,
    scale_ref,
    resid_ref,
    sems,
):
    rows, window, width = kv_ref.shape
    piece = rows // KV_PIECES
    copies = [
        pltpu.make_async_copy(src, dst, sems.at[i])
        for i, (src, dst) in enumerate(
            [
                (q_hbm, q_ref),
                (new_hbm, new_ref),
                (pos_hbm, pos_ref),
                (sink_hbm, sink_ref),
                (ids_hbm, ids_ref),
                (scale_hbm, scale_ref),
                (resid_hbm, resid_ref),
            ]
        )
    ]
    first = len(copies)
    kv_copies = [
        pltpu.make_async_copy(
            kv_hbm.at[pl.ds(i * piece, piece)], kv_ref.at[pl.ds(i * piece, piece)], sems.at[first + i]
        )
        for i in range(KV_PIECES)
    ]
    proj_copy = pltpu.make_async_copy(proj_hbm, proj_ref, sems.at[first + KV_PIECES])
    for copy in copies + kv_copies:
        copy.start()
    proj_copy.start()
    for copy in copies:
        copy.wait()

    line = lax.broadcasted_iota(jnp.int32, pick_ref.shape, 0)
    named = jnp.zeros(pick_ref.shape, jnp.float32)
    weighted = jnp.zeros(pick_ref.shape, jnp.float32)
    for k in range(ids_ref.shape[0]):
        match = ids_ref[k : k + 1, :] == line // 2
        named = jnp.where(match, 1.0, named)
        weighted = jnp.where(
            match, scale_ref[k : k + 1, :].astype(jnp.float32) / 65536.0, weighted
        )
    ahead = lax.broadcasted_iota(jnp.int32, (rows, rows), 0) < lax.broadcasted_iota(
        jnp.int32, (rows, rows), 1
    )
    before = jnp.dot(
        named, ahead.astype(jnp.float32), preferred_element_type=jnp.float32
    ).astype(jnp.int32)
    kept = before == line % 2
    pick_ref[...] = jnp.where(kept, named, 0.0).astype(jnp.bfloat16)
    combine_ref[...] = jnp.where(kept, weighted, 0.0)
    width_here = share_ref.shape[1]
    here = lax.axis_index("y") * 2 + lax.axis_index("core")
    for s in range(out_ref.shape[0]):

        @pl.when(here == s)
        def _(s=s):
            share_ref[...] = resid_ref[:, s * width_here : (s + 1) * width_here]

    half = width // 2
    groups = 4
    shares, _, share_width = out_ref.shape
    lane = lax.broadcasted_iota(jnp.int32, (rows, width), 1)
    row = lax.broadcasted_iota(jnp.int32, (rows, width), 0)
    low = lane < half
    q = q_ref[...].astype(jnp.float32)
    parts = []
    for pair in range(groups // 2):
        both = q[:, pair * width : (pair + 1) * width]
        parts.append(jnp.where(low, both, 0.0))
        parts.append(jnp.where(low, pltpu.roll(both, half, 1), 0.0))
    stacked = jnp.concatenate(parts, axis=0)
    stacked_low = stacked.astype(jnp.bfloat16)
    new = new_ref[...].astype(jnp.float32)
    new_all = jnp.concatenate([new] * groups, axis=0)

    pos = jnp.zeros((rows, width), jnp.int32)
    for t in range(rows):
        pos = jnp.where(row == t, pos_ref[t], pos)
    pos = jnp.concatenate([pos] * groups, axis=0)
    lanes = lax.broadcasted_iota(jnp.int32, pos.shape, 1)
    request = lax.broadcasted_iota(jnp.int32, pos.shape, 0) % rows
    group = lax.broadcasted_iota(jnp.int32, (groups * rows, 1), 0) // rows
    sink = jnp.zeros((groups * rows, 1), jnp.float32)
    for g in range(groups):
        sink = jnp.where(group == g, sink_ref[0, g], sink)

    scores = jnp.zeros((groups * rows, window), jnp.float32)
    for t in range(rows):
        if t % piece == 0:
            kv_copies[t // piece].wait()
        found = lax.dot_general(
            stacked_low, kv_ref[t], (((1,), (1,)), ((), ())), preferred_element_type=jnp.float32
        )
        scores = jnp.where(request == t, found, scores)
    newest = jnp.sum(stacked * new_all, axis=1, keepdims=True)
    is_new = lanes == (pos & (window - 1))
    scores = jnp.where(is_new, newest, scores) * (half**-0.5)
    scores = jnp.where(lanes <= pos, scores, -jnp.inf)
    largest = jnp.maximum(jnp.max(scores, axis=1, keepdims=True), sink)
    raised = jnp.exp(scores - largest)
    total = jnp.sum(raised, axis=1, keepdims=True) + jnp.exp(sink - largest)
    weights = (raised / total).astype(jnp.bfloat16).astype(jnp.float32)
    newest_weight = jnp.sum(jnp.where(is_new, weights, 0.0), axis=1, keepdims=True)
    older = jnp.where(is_new, 0.0, weights).astype(jnp.bfloat16)
    mixed = jnp.zeros((groups * rows, width), jnp.float32)
    for t in range(rows):
        found = jnp.dot(older, kv_ref[t], preferred_element_type=jnp.float32)
        mixed = jnp.where(request == t, found, mixed)
    mixed = mixed + newest_weight * new_all
    merged = []
    for pair in range(groups // 2):
        first = mixed[2 * pair * rows : (2 * pair + 1) * rows]
        second = mixed[(2 * pair + 1) * rows : (2 * pair + 2) * rows]
        merged.append(jnp.where(low, pltpu.roll(first, half, 1), second))
    merged = jnp.concatenate(merged, axis=1).astype(jnp.bfloat16)
    proj_copy.wait()
    for s in range(shares):
        out_ref[s] = lax.dot_general(
            merged,
            proj_ref[pl.ds(s * share_width, share_width), :],
            (((1,), (1,)), ((), ())),
            preferred_element_type=jnp.float32,
        ).astype(jnp.bfloat16)


def attend(
    positions, sink_logits, queries, kv_cache, new_kv, out_proj, route_ids, route_weights, residual
):
    rows, _, window, width = kv_cache.shape
    slots = 2 * lax.axis_size(GRP)
    features = out_proj.shape[2]
    hbm = pl.BlockSpec(memory_space=pltpu.HBM)
    return pl.pallas_call(
        attend_kernel,
        out_shape=(
            jax.ShapeDtypeStruct((8, rows, features // 8), jnp.bfloat16),
            jax.ShapeDtypeStruct((slots, rows), jnp.bfloat16),
            jax.ShapeDtypeStruct((slots, rows), jnp.float32),
            jax.ShapeDtypeStruct((rows, features // 8), jnp.bfloat16),
        ),
        in_specs=[hbm] * 9,
        out_specs=(pl.BlockSpec(memory_space=pltpu.VMEM),) * 4,
        scratch_shapes=[
            pltpu.SMEM((rows,), jnp.int32),
            pltpu.SMEM(sink_logits.shape, jnp.float32),
            pltpu.VMEM((rows, queries.shape[2]), jnp.bfloat16),
            pltpu.VMEM((rows, window, width), jnp.bfloat16),
            pltpu.VMEM((rows, width), jnp.bfloat16),
            pltpu.VMEM((features, out_proj.shape[1]), jnp.bfloat16),
            pltpu.VMEM(route_ids.shape[::-1], jnp.int32),
            pltpu.VMEM(route_weights.shape[::-1], jnp.int32),
            pltpu.VMEM(residual.shape, jnp.bfloat16),
            pltpu.SemaphoreType.DMA((8 + KV_PIECES,)),
        ],
        compiler_params=pltpu.CompilerParams(vmem_limit_bytes=8 * MIB),
        name="attend",
    )(
        *(
            pltpu.with_memory_space_constraint(x, pltpu.HBM)
            for x in (
                positions,
                sink_logits,
                queries.reshape(rows, -1),
                kv_cache.reshape(rows, window, width),
                new_kv.reshape(rows, width),
                jnp.swapaxes(out_proj[0], 0, 1),
                route_ids.T,
                route_weights.T,
                residual,
            )
        )
    )


def fold_kernel(w_ref, gain_ref, out_ref):
    out_ref[...] = (w_ref[...].astype(jnp.float32) * gain_ref[...]).astype(jnp.bfloat16)


def expert_kernel(x_ref, w_ref, down_ref, send_ref, own_ref, held_ref):
    x = x_ref[...]
    wide = x.astype(jnp.float32)
    mean_square = jnp.mean(wide * wide, axis=0, keepdims=True)
    projected = jnp.dot(w_ref[...], x, preferred_element_type=jnp.float32)
    held_ref[...] = projected * lax.rsqrt(mean_square + epsilon)
    units = held_ref.shape[0] // 2
    gate = held_ref[pl.ds(0, units, stride=2), :]
    up = held_ref[pl.ds(1, units, stride=2), :]
    act = ((up + 1.0) * gate * jax.nn.sigmoid(swish_alpha * gate)).astype(jnp.bfloat16)
    partial = lax.dot_general(
        act, down_ref[...], (((0,), (0,)), ((), ())), preferred_element_type=jnp.float32
    )
    y_size = send_ref.shape[0]
    share = down_ref.shape[1] // (2 * y_size)
    for c in range(2):

        @pl.when(lax.axis_index("core") == c)
        def _(c=c):
            for y in range(y_size):
                start = (2 * y + 1 - c) * share
                send_ref[y, :, :share] = partial[:, start : start + share].astype(jnp.bfloat16)
                start = (2 * y + c) * share
                own_ref[y, :, :share] = partial[:, start : start + share]


def local(
    residual,
    queries,
    kv_cache,
    new_kv,
    positions,
    sink_logits,
    out_proj,
    norm_gain,
    route_ids,
    route_weights,
    w_gate_up,
    w_down,
):
    rows, features = residual.shape
    experts = lax.axis_size(GRP)
    shares = lax.axis_size(HEAD)
    y_size = lax.axis_size("y")
    share = features // shares
    capacity = 2
    slots = experts * capacity
    units = w_down.shape[1]
    vmem = pl.BlockSpec(memory_space=pltpu.VMEM)

    parts, pick, combine, resid_here = attend(
        positions,
        sink_logits,
        queries,
        kv_cache,
        new_kv,
        out_proj,
        route_ids,
        route_weights,
        residual,
    )
    parts = lax.all_to_all(parts, HEAD, 0, 0, tiled=True)
    attention = jnp.sum(parts.astype(jnp.float32), axis=0)
    hidden = (resid_here.astype(jnp.float32) + attention).astype(jnp.bfloat16)

    outgoing = jnp.dot(pick, hidden, preferred_element_type=jnp.float32).astype(jnp.bfloat16)
    got = lax.all_to_all(outgoing.reshape(experts, capacity, share), GRP, 0, 0, tiled=True)
    got = jnp.swapaxes(got.reshape(slots, share), 0, 1)
    mine = lax.all_to_all(
        jnp.broadcast_to(got[None], (y_size, share, slots)), "y", 0, 0, tiled=True
    )
    gate_up, gain, mine = lax.optimization_barrier(
        (jnp.swapaxes(w_gate_up[0], 0, 1), norm_gain, mine)
    )
    gate_up = pl.pallas_call(
        fold_kernel,
        out_shape=jax.ShapeDtypeStruct(gate_up.shape, jnp.bfloat16),
        in_specs=[vmem, vmem],
        out_specs=vmem,
        compiler_params=pltpu.CompilerParams(vmem_limit_bytes=16 * MIB),
        name="fold",
    )(gate_up, gain.reshape(1, -1))
    swap = [(0, 1), (1, 0)]
    theirs = lax.ppermute(mine, "core", swap)
    is_low = lax.axis_index("core") == 0
    full = jnp.stack(
        [jnp.where(is_low, mine, theirs), jnp.where(is_low, theirs, mine)], axis=1
    ).reshape(features, slots)

    lanes = pl.cdiv(share, 128) * 128
    sent, own = pl.pallas_call(
        expert_kernel,
        out_shape=(
            jax.ShapeDtypeStruct((y_size, slots, lanes), jnp.bfloat16),
            jax.ShapeDtypeStruct((y_size, slots, lanes), jnp.float32),
        ),
        in_specs=[vmem, vmem, vmem],
        out_specs=(vmem, vmem),
        scratch_shapes=[pltpu.VMEM((2 * units, slots), jnp.float32)],
        compiler_params=pltpu.CompilerParams(vmem_limit_bytes=16 * MIB),
        name="expert",
    )(full, gate_up, w_down[0])
    arrived = lax.ppermute(sent, "core", swap)
    paired = (own + arrived.astype(jnp.float32)).astype(jnp.bfloat16)
    paired = lax.all_to_all(paired, "y", 0, 0, tiled=True)
    summed = jnp.sum(paired[:, :, :share].astype(jnp.float32), axis=0).astype(jnp.bfloat16)
    back = lax.all_to_all(
        summed.reshape(experts, capacity, share), GRP, 0, 0, tiled=True
    )
    mixture = lax.dot_general(
        combine,
        back.reshape(slots, share).astype(jnp.float32),
        (((0,), (0,)), ((), ())),
        precision=lax.Precision.HIGHEST,
    )
    return (hidden.astype(jnp.float32) + mixture).astype(jnp.bfloat16)


def solution(mesh):
    fine = Mesh(mesh.devices.reshape(GRID), ("z", "x", "y", "core"))
    in_specs = (
        P(GRP, None),
        P(GRP, HEAD, None),
        P(GRP, HEAD, None, None),
        P(GRP, HEAD, None),
        P(GRP),
        P(HEAD, None),
        P(HEAD, None, None),
        P(),
        P(GRP, None),
        P(GRP, None),
        P(GRP, None, HEAD),
        P(GRP, HEAD, None),
    )
    return jax.shard_map(
        local, mesh=fine, in_specs=in_specs, out_specs=P(GRP, HEAD), check_vma=False
    )
```

```python
import jax
import jax.numpy as jnp
from jax import lax
from jax.experimental import pallas as pl
from jax.experimental.pallas import tpu as pltpu
from jax.sharding import Mesh, PartitionSpec as P

epsilon = 1e-05
swish_alpha = 1.702

GRID = (16, 4, 4, 2)
GRP = ("z", "x")
HEAD = ("y", "core")
FEATURES = 2880
MIB = 1 << 20
KV_PIECES = 4
PROJ_PIECES = 4


def attend_kernel(
    pos_hbm,
    sink_hbm,
    q_hbm,
    kv_hbm,
    new_hbm,
    proj_hbm,
    ids_hbm,
    scale_hbm,
    resid_hbm,
    out_ref,
    pick_ref,
    combine_ref,
    share_ref,
    pos_ref,
    sink_ref,
    q_ref,
    kv_ref,
    new_ref,
    proj_ref,
    ids_ref,
    scale_ref,
    resid_ref,
    sems,
):
    rows, window, width = kv_ref.shape
    piece = rows // KV_PIECES
    copies = [
        pltpu.make_async_copy(src, dst, sems.at[i])
        for i, (src, dst) in enumerate(
            [
                (q_hbm, q_ref),
                (new_hbm, new_ref),
                (pos_hbm, pos_ref),
                (sink_hbm, sink_ref),
                (ids_hbm, ids_ref),
                (scale_hbm, scale_ref),
                (resid_hbm, resid_ref),
            ]
        )
    ]
    first = len(copies)
    kv_copies = [
        pltpu.make_async_copy(
            kv_hbm.at[pl.ds(i * piece, piece)], kv_ref.at[pl.ds(i * piece, piece)], sems.at[first + i]
        )
        for i in range(KV_PIECES)
    ]
    shares = out_ref.shape[0]
    part = proj_ref.shape[0] // PROJ_PIECES
    proj_copies = [
        pltpu.make_async_copy(
            proj_hbm.at[pl.ds(i * part, part)],
            proj_ref.at[pl.ds(i * part, part)],
            sems.at[first + KV_PIECES + i],
        )
        for i in range(PROJ_PIECES)
    ]
    for copy in copies + kv_copies + proj_copies:
        copy.start()
    for copy in copies:
        copy.wait()

    line = lax.broadcasted_iota(jnp.int32, pick_ref.shape, 0)
    named = jnp.zeros(pick_ref.shape, jnp.float32)
    weighted = jnp.zeros(pick_ref.shape, jnp.float32)
    for k in range(ids_ref.shape[0]):
        match = ids_ref[k : k + 1, :] == line // 2
        named = jnp.where(match, 1.0, named)
        weighted = jnp.where(
            match, scale_ref[k : k + 1, :].astype(jnp.float32) / 65536.0, weighted
        )
    ahead = lax.broadcasted_iota(jnp.int32, (rows, rows), 0) < lax.broadcasted_iota(
        jnp.int32, (rows, rows), 1
    )
    before = jnp.dot(
        named, ahead.astype(jnp.float32), preferred_element_type=jnp.float32
    ).astype(jnp.int32)
    kept = before == line % 2
    pick_ref[...] = jnp.where(kept, named, 0.0).astype(jnp.bfloat16)
    combine_ref[...] = jnp.where(kept, weighted, 0.0)
    width_here = share_ref.shape[1]
    here = lax.axis_index("y") * 2 + lax.axis_index("core")
    for s in range(out_ref.shape[0]):

        @pl.when(here == s)
        def _(s=s):
            share_ref[...] = resid_ref[:, s * width_here : (s + 1) * width_here]

    half = width // 2
    groups = 4
    share_width = out_ref.shape[2]
    lane = lax.broadcasted_iota(jnp.int32, (rows, width), 1)
    row = lax.broadcasted_iota(jnp.int32, (rows, width), 0)
    low = lane < half
    q = q_ref[...].astype(jnp.float32)
    parts = []
    for pair in range(groups // 2):
        both = q[:, pair * width : (pair + 1) * width]
        parts.append(jnp.where(low, both, 0.0))
        parts.append(jnp.where(low, pltpu.roll(both, half, 1), 0.0))
    stacked = jnp.concatenate(parts, axis=0)
    stacked_low = stacked.astype(jnp.bfloat16)
    new = new_ref[...].astype(jnp.float32)
    new_all = jnp.concatenate([new] * groups, axis=0)

    pos = jnp.zeros((rows, width), jnp.int32)
    for t in range(rows):
        pos = jnp.where(row == t, pos_ref[t], pos)
    pos = jnp.concatenate([pos] * groups, axis=0)
    lanes = lax.broadcasted_iota(jnp.int32, pos.shape, 1)
    request = lax.broadcasted_iota(jnp.int32, pos.shape, 0) % rows
    group = lax.broadcasted_iota(jnp.int32, (groups * rows, 1), 0) // rows
    sink = jnp.zeros((groups * rows, 1), jnp.float32)
    for g in range(groups):
        sink = jnp.where(group == g, sink_ref[0, g], sink)

    scores = jnp.zeros((groups * rows, window), jnp.float32)
    for t in range(rows):
        if t % piece == 0:
            kv_copies[t // piece].wait()
        found = lax.dot_general(
            stacked_low, kv_ref[t], (((1,), (1,)), ((), ())), preferred_element_type=jnp.float32
        )
        scores = jnp.where(request == t, found, scores)
    newest = jnp.sum(stacked * new_all, axis=1, keepdims=True)
    is_new = lanes == (pos & (window - 1))
    scores = jnp.where(is_new, newest, scores) * (half**-0.5)
    scores = jnp.where(lanes <= pos, scores, -jnp.inf)
    largest = jnp.maximum(jnp.max(scores, axis=1, keepdims=True), sink)
    raised = jnp.exp(scores - largest)
    total = jnp.sum(raised, axis=1, keepdims=True) + jnp.exp(sink - largest)
    weights = (raised / total).astype(jnp.bfloat16).astype(jnp.float32)
    newest_weight = jnp.sum(jnp.where(is_new, weights, 0.0), axis=1, keepdims=True)
    older = jnp.where(is_new, 0.0, weights).astype(jnp.bfloat16)
    mixed = jnp.zeros((groups * rows, width), jnp.float32)
    for t in range(rows):
        found = jnp.dot(older, kv_ref[t], preferred_element_type=jnp.float32)
        mixed = jnp.where(request == t, found, mixed)
    mixed = mixed + newest_weight * new_all
    merged = []
    for pair in range(groups // 2):
        first = mixed[2 * pair * rows : (2 * pair + 1) * rows]
        second = mixed[(2 * pair + 1) * rows : (2 * pair + 2) * rows]
        merged.append(jnp.where(low, pltpu.roll(first, half, 1), second))
    merged = jnp.concatenate(merged, axis=1).astype(jnp.bfloat16)
    for s in range(shares):
        if s % (shares // PROJ_PIECES) == 0:
            proj_copies[s // (shares // PROJ_PIECES)].wait()
        out_ref[s] = lax.dot_general(
            merged,
            proj_ref[pl.ds(s * share_width, share_width), :],
            (((1,), (1,)), ((), ())),
            preferred_element_type=jnp.float32,
        ).astype(jnp.bfloat16)


def attend(
    positions, sink_logits, queries, kv_cache, new_kv, out_proj, route_ids, route_weights, residual
):
    rows, _, window, width = kv_cache.shape
    slots = 2 * lax.axis_size(GRP)
    features = out_proj.shape[2]
    hbm = pl.BlockSpec(memory_space=pltpu.HBM)
    return pl.pallas_call(
        attend_kernel,
        out_shape=(
            pltpu.VMEM((8, rows, features // 8), jnp.bfloat16),
            pltpu.VMEM((slots, rows), jnp.bfloat16),
            pltpu.VMEM((slots, rows), jnp.float32),
            pltpu.VMEM((rows, features // 8), jnp.bfloat16),
        ),
        in_specs=[hbm] * 9,
        out_specs=(pl.BlockSpec(memory_space=pltpu.VMEM),) * 4,
        scratch_shapes=[
            pltpu.SMEM((rows,), jnp.int32),
            pltpu.SMEM(sink_logits.shape, jnp.float32),
            pltpu.VMEM((rows, queries.shape[2]), jnp.bfloat16),
            pltpu.VMEM((rows, window, width), jnp.bfloat16),
            pltpu.VMEM((rows, width), jnp.bfloat16),
            pltpu.VMEM((features, out_proj.shape[1]), jnp.bfloat16),
            pltpu.VMEM(route_ids.shape[::-1], jnp.int32),
            pltpu.VMEM(route_weights.shape[::-1], jnp.int32),
            pltpu.VMEM(residual.shape, jnp.bfloat16),
            pltpu.SemaphoreType.DMA((7 + KV_PIECES + PROJ_PIECES,)),
        ],
        compiler_params=pltpu.CompilerParams(vmem_limit_bytes=int(61.4 * MIB)),
        name="attend",
    )(
        *(
            pltpu.with_memory_space_constraint(x, pltpu.HBM)
            for x in (
                positions,
                sink_logits,
                queries.reshape(rows, -1),
                kv_cache.reshape(rows, window, width),
                new_kv.reshape(rows, width),
                jnp.swapaxes(out_proj[0], 0, 1),
                route_ids.T,
                route_weights.T,
                residual,
            )
        )
    )


def dispatch_kernel(parts_ref, share_ref, pick_ref, hidden_ref, out_ref):
    summed = jnp.sum(parts_ref[...].astype(jnp.float32), axis=0)
    hidden = (share_ref[...].astype(jnp.float32) + summed).astype(jnp.bfloat16)
    hidden_ref[...] = hidden
    out_ref[...] = jnp.dot(
        pick_ref[...], hidden, preferred_element_type=jnp.float32
    ).astype(jnp.bfloat16)


def swap_rows(rows, outer, inner):
    count = rows.shape[0]
    to = lax.broadcasted_iota(jnp.int32, (count, count), 0)
    at = lax.broadcasted_iota(jnp.int32, (count, count), 1)
    source = ((to // 2) % outer) * (2 * inner) + (to // (2 * outer)) * 2 + to % 2
    return jnp.dot(
        (at == source).astype(jnp.bfloat16), rows, preferred_element_type=jnp.float32
    ).astype(jnp.bfloat16)


def spread_kernel(got_ref, out_ref):
    z_size, x_size = GRID[0], GRID[1]
    share = got_ref.shape[1]
    rows = swap_rows(got_ref[...], z_size, x_size)
    rest = jnp.zeros((rows.shape[0], out_ref.shape[2] - share), jnp.bfloat16)
    for y in range(out_ref.shape[0]):
        out_ref[y, :, :share] = rows
        out_ref[y, :, share:] = rest


def gather_kernel(parts_ref, out_ref):
    z_size, x_size = GRID[0], GRID[1]
    share = out_ref.shape[1]
    summed = jnp.sum(parts_ref[...].astype(jnp.float32), axis=0)[:, :share]
    out_ref[...] = swap_rows(summed.astype(jnp.bfloat16), x_size, z_size)


def relay_kernel(up_ref, gain_ref, down_hbm, up_out, down_out, down_ref, sem):
    copy = pltpu.make_async_copy(down_hbm, down_ref, sem)
    copy.start()
    y_size = GRID[2]
    share = down_ref.shape[1] // (2 * y_size)
    lanes = down_out.shape[2] // y_size

    def lay(source, out):
        rest = jnp.zeros((source.shape[0], lanes - share), jnp.bfloat16)
        for y in range(y_size):
            for c in range(2):
                start = (2 * y + c) * share
                out[c, :, y * lanes : y * lanes + share] = source[:, start : start + share]
                out[c, :, y * lanes + share : (y + 1) * lanes] = rest

    lay((up_ref[...].astype(jnp.float32) * gain_ref[...]).astype(jnp.bfloat16), up_out)
    copy.wait()
    lay(down_ref[...], down_out)


def joined(ref):
    return jnp.concatenate([ref[y] for y in range(ref.shape[0])], axis=1)


def expert_kernel(mine_ref, theirs_ref, up_ref, down_ref, act_ref, send_ref, held_ref):
    core = lax.axis_index("core")
    y_size, slots, lanes = mine_ref.shape
    units = act_ref.shape[0]
    projected = jnp.zeros(held_ref.shape, jnp.float32)
    squares = jnp.zeros((slots, 128), jnp.float32)
    for ref, index in ((mine_ref, core), (theirs_ref, 1 - core)):
        x = joined(ref)
        projected = projected + lax.dot_general(
            up_ref[index], x, (((1,), (1,)), ((), ())), preferred_element_type=jnp.float32
        )
        wide = x.astype(jnp.float32)
        wide = wide * wide
        for tile in range(wide.shape[1] // 128):
            squares = squares + wide[:, tile * 128 : (tile + 1) * 128]
    mean_square = jnp.sum(jnp.transpose(squares), axis=0, keepdims=True) / FEATURES
    held_ref[...] = projected * lax.rsqrt(mean_square + epsilon)
    gate = held_ref[pl.ds(0, units, stride=2), :]
    up = held_ref[pl.ds(1, units, stride=2), :]
    act = ((up + 1.0) * gate * jax.nn.sigmoid(swish_alpha * gate)).astype(jnp.bfloat16)
    act_ref[...] = act
    partial = lax.dot_general(
        act, down_ref[1 - core], (((0,), (0,)), ((), ())), preferred_element_type=jnp.float32
    ).astype(jnp.bfloat16)
    for y in range(y_size):
        send_ref[y] = partial[:, y * lanes : (y + 1) * lanes]


def own_kernel(act_ref, down_ref, out_ref):
    y_size, _, lanes = out_ref.shape
    partial = lax.dot_general(
        act_ref[...],
        down_ref[lax.axis_index("core")],
        (((0,), (0,)), ((), ())),
        preferred_element_type=jnp.float32,
    )
    for y in range(y_size):
        out_ref[y] = partial[:, y * lanes : (y + 1) * lanes]


def run(kernel, name, outs, scratch=(), from_hbm=()):
    vmem = pl.BlockSpec(memory_space=pltpu.VMEM)
    hbm = pl.BlockSpec(memory_space=pltpu.HBM)

    def call(*operands):
        return pl.pallas_call(
            kernel,
            out_shape=tuple(pltpu.VMEM(shape, dtype) for shape, dtype in outs),
            in_specs=[hbm if i in from_hbm else vmem for i in range(len(operands))],
            out_specs=(vmem,) * len(outs),
            scratch_shapes=list(scratch),
            compiler_params=pltpu.CompilerParams(vmem_limit_bytes=16 * MIB),
            name=name,
        )(*operands)

    return call


def local(
    residual,
    queries,
    kv_cache,
    new_kv,
    positions,
    sink_logits,
    out_proj,
    norm_gain,
    route_ids,
    route_weights,
    w_gate_up,
    w_down,
):
    rows, features = residual.shape
    z_size, x_size, y_size, _ = GRID
    share = features // (2 * y_size)
    lanes = pl.cdiv(share, 128) * 128
    slots = 2 * z_size * x_size
    units = w_down.shape[1]
    bf16 = jnp.bfloat16
    plane = ("y", "x")
    swap = [(0, 1), (1, 0)]

    parts, pick, combine, resid_here = attend(
        positions,
        sink_logits,
        queries,
        kv_cache,
        new_kv,
        out_proj,
        route_ids,
        route_weights,
        residual,
    )
    parts = lax.all_to_all(parts, HEAD, 0, 0, tiled=True)
    hidden, outgoing = run(
        dispatch_kernel, "dispatch", [((rows, share), bf16), ((slots, share), bf16)]
    )(parts, resid_here, pick)

    got = lax.all_to_all(outgoing.reshape(z_size, 2 * x_size, share), "z", 0, 0, tiled=True)
    (spread,) = run(spread_kernel, "spread", [((y_size, slots, lanes), bf16)])(
        got.reshape(slots, share)
    )
    mine = lax.all_to_all(
        spread.reshape(y_size * x_size, 2 * z_size, lanes), plane, 0, 0, tiled=True
    ).reshape(y_size, slots, lanes)
    gate_up, down, gain, mine = lax.optimization_barrier(
        (jnp.swapaxes(w_gate_up[0], 0, 1), w_down[0], norm_gain, mine)
    )
    gate_up, down = run(
        relay_kernel,
        "relay",
        [((2, 2 * units, y_size * lanes), bf16), ((2, units, y_size * lanes), bf16)],
        [pltpu.VMEM((units, features), bf16), pltpu.SemaphoreType.DMA],
        from_hbm=(2,),
    )(gate_up, gain.reshape(1, -1), pltpu.with_memory_space_constraint(down, pltpu.HBM))
    theirs = lax.ppermute(mine, "core", swap)
    act, sent = run(
        expert_kernel,
        "expert",
        [((units, slots), bf16), ((y_size, slots, lanes), bf16)],
        [pltpu.VMEM((2 * units, slots), jnp.float32)],
    )(mine, theirs, gate_up, down)

    arrived = lax.ppermute(sent, "core", swap)
    (own,) = run(own_kernel, "own", [((y_size, slots, lanes), jnp.float32)])(act, down)
    paired = (own + arrived.astype(jnp.float32)).astype(bf16)
    paired = lax.all_to_all(
        paired.reshape(y_size * x_size, 2 * z_size, lanes), plane, 0, 0, tiled=True
    )
    (summed,) = run(gather_kernel, "gather", [((slots, share), bf16)])(
        paired.reshape(y_size, slots, lanes)
    )
    back = lax.all_to_all(summed.reshape(z_size, 2 * x_size, share), "z", 0, 0, tiled=True)
    mixture = lax.dot_general(
        combine,
        back.reshape(slots, share).astype(jnp.float32),
        (((0,), (0,)), ((), ())),
        precision=lax.Precision.HIGHEST,
    )
    return (hidden.astype(jnp.float32) + mixture).astype(bf16)


def solution(mesh):
    fine = Mesh(mesh.devices.reshape(GRID), ("z", "x", "y", "core"))
    in_specs = (
        P(GRP, None),
        P(GRP, HEAD, None),
        P(GRP, HEAD, None, None),
        P(GRP, HEAD, None),
        P(GRP),
        P(HEAD, None),
        P(HEAD, None, None),
        P(),
        P(GRP, None),
        P(GRP, None),
        P(GRP, None, HEAD),
        P(GRP, HEAD, None),
    )
    return jax.shard_map(
        local, mesh=fine, in_specs=in_specs, out_specs=P(GRP, HEAD), check_vma=False
    )
```

```python
import jax
import jax.numpy as jnp
from jax import lax
from jax.experimental import pallas as pl
from jax.experimental.pallas import tpu as pltpu
from jax.sharding import Mesh, PartitionSpec as P

epsilon = 1e-05
swish_alpha = 1.702

GRID = (16, 4, 4, 2)
GRP = ("z", "x")
HEAD = ("y", "core")
PLANE = ("y", "x")
FEATURES = 2880
MIB = 1 << 20


def attend_kernel(
    pos_hbm,
    sink_hbm,
    q_hbm,
    kv_hbm,
    new_hbm,
    proj_hbm,
    out_ref,
    pos_ref,
    sink_ref,
    q_ref,
    kv_ref,
    new_ref,
    proj_ref,
    sems,
):
    rows, window, width = kv_ref.shape
    shares = out_ref.shape[0]
    q_copy, kv_copy, new_copy, pos_copy, sink_copy, proj_copy = (
        pltpu.make_async_copy(src, dst, sems.at[i])
        for i, (src, dst) in enumerate(
            [
                (q_hbm, q_ref),
                (kv_hbm, kv_ref),
                (new_hbm, new_ref),
                (pos_hbm, pos_ref),
                (sink_hbm, sink_ref),
                (proj_hbm, proj_ref),
            ]
        )
    )
    for copy in (q_copy, kv_copy, new_copy, pos_copy, sink_copy, proj_copy):
        copy.start()
    half = width // 2
    groups = 4
    share_width = out_ref.shape[2]
    lane = lax.broadcasted_iota(jnp.int32, (rows, width), 1)
    low = lane < half
    q_copy.wait()
    q = q_ref[...].astype(jnp.float32)
    parts = []
    for pair in range(groups // 2):
        both = q[:, pair * width : (pair + 1) * width]
        parts.append(jnp.where(low, both, 0.0))
        parts.append(jnp.where(low, pltpu.roll(both, half, 1), 0.0))
    stacked = jnp.concatenate(parts, axis=0)
    stacked_low = stacked.astype(jnp.bfloat16)
    shape = (groups * rows, window)
    lanes = lax.broadcasted_iota(jnp.int32, shape, 1)
    request = lax.broadcasted_iota(jnp.int32, shape, 0) % rows

    kv_copy.wait()
    kv = kv_ref[...].reshape(rows * window, width)
    found = lax.dot_general(
        stacked_low, kv, (((1,), (1,)), ((), ())), preferred_element_type=jnp.float32
    )
    scores = jnp.zeros(shape, jnp.float32)
    for t in range(rows):
        scores = jnp.where(request == t, found[:, t * window : (t + 1) * window], scores)
    for copy in (new_copy, pos_copy, sink_copy):
        copy.wait()
    new = new_ref[...].astype(jnp.float32)
    new_all = jnp.concatenate([new] * groups, axis=0)
    square = (rows, rows)
    diagonal = lax.broadcasted_iota(jnp.int32, square, 0) == lax.broadcasted_iota(
        jnp.int32, square, 1
    )
    pos = jnp.sum(jnp.where(diagonal, pos_ref[...], 0), axis=1, keepdims=True)
    pos = jnp.concatenate([jnp.broadcast_to(pos, (rows, width))] * groups, axis=0)
    heads = (groups * rows, groups)
    of_head = lax.broadcasted_iota(jnp.int32, heads, 0) // rows == lax.broadcasted_iota(
        jnp.int32, heads, 1
    )
    sink = jnp.sum(jnp.where(of_head, sink_ref[...], 0.0), axis=1, keepdims=True)
    newest = jnp.sum(stacked * new_all, axis=1, keepdims=True)
    is_new = lanes == (pos & (window - 1))
    scores = jnp.where(is_new, newest, scores) * (half**-0.5)
    scores = jnp.where(lanes <= pos, scores, -jnp.inf)
    largest = jnp.maximum(jnp.max(scores, axis=1, keepdims=True), sink)
    raised = jnp.exp(scores - largest)
    total = jnp.sum(raised, axis=1, keepdims=True) + jnp.exp(sink - largest)
    weights = (raised / total).astype(jnp.bfloat16).astype(jnp.float32)
    newest_weight = jnp.sum(jnp.where(is_new, weights, 0.0), axis=1, keepdims=True)
    older = jnp.where(is_new, 0.0, weights)
    spread = jnp.concatenate(
        [jnp.where(request == t, older, 0.0).astype(jnp.bfloat16) for t in range(rows)], axis=1
    )
    mixed = jnp.dot(spread, kv, preferred_element_type=jnp.float32)
    mixed = mixed + newest_weight * new_all
    merged = []
    for pair in range(groups // 2):
        even = mixed[2 * pair * rows : (2 * pair + 1) * rows]
        odd = mixed[(2 * pair + 1) * rows : (2 * pair + 2) * rows]
        merged.append(jnp.where(low, pltpu.roll(even, half, 1), odd))
    merged = jnp.concatenate(merged, axis=1).astype(jnp.bfloat16)
    proj_copy.wait()
    for s in range(shares):
        out_ref[s] = lax.dot_general(
            merged,
            proj_ref[pl.ds(s * share_width, share_width), :],
            (((1,), (1,)), ((), ())),
            preferred_element_type=jnp.float32,
        ).astype(jnp.bfloat16)


def attend(positions, sink_logits, queries, kv_cache, new_kv, out_proj):
    rows, _, window, width = kv_cache.shape
    features = out_proj.shape[2]
    hbm = pl.BlockSpec(memory_space=pltpu.HBM)
    return pl.pallas_call(
        attend_kernel,
        out_shape=pltpu.VMEM((8, rows, features // 8), jnp.bfloat16),
        in_specs=[hbm] * 6,
        out_specs=pl.BlockSpec(memory_space=pltpu.VMEM),
        scratch_shapes=[
            pltpu.VMEM((1, rows), jnp.int32),
            pltpu.VMEM(sink_logits.shape, jnp.float32),
            pltpu.VMEM((rows, queries.shape[2]), jnp.bfloat16),
            pltpu.VMEM((rows, window, width), jnp.bfloat16),
            pltpu.VMEM((rows, width), jnp.bfloat16),
            pltpu.VMEM((features, out_proj.shape[1]), jnp.bfloat16),
            pltpu.SemaphoreType.DMA((6,)),
        ],
        compiler_params=pltpu.CompilerParams(vmem_limit_bytes=16 * MIB),
        name="attend",
    )(
        *(
            pltpu.with_memory_space_constraint(x, pltpu.HBM)
            for x in (
                positions.reshape(1, rows),
                sink_logits,
                queries.reshape(rows, -1),
                kv_cache.reshape(rows, window, width),
                new_kv.reshape(rows, width),
                jnp.swapaxes(out_proj[0], 0, 1),
            )
        )
    )


def dispatch_kernel(
    parts_ref,
    ids_ref,
    scale_ref,
    resid_ref,
    gain_ref,
    later_hbm,
    hidden_ref,
    out_ref,
    combine_ref,
    share_ref,
    gain_here_ref,
    row_ref,
):
    rows, share_width = hidden_ref.shape
    gain = gain_ref[...][None, :]
    here = 2 * lax.axis_index("y") + lax.axis_index("core")
    for s in range(parts_ref.shape[0]):

        @pl.when(here == s)
        def _(s=s):
            share_ref[...] = resid_ref[:, s * share_width : (s + 1) * share_width]
            gain_here_ref[...] = gain[:, s * share_width : (s + 1) * share_width]

    line = lax.broadcasted_iota(jnp.int32, combine_ref.shape, 0)
    named = jnp.zeros(combine_ref.shape, jnp.float32)
    weighted = jnp.zeros(combine_ref.shape, jnp.float32)
    for k in range(ids_ref.shape[0]):
        match = ids_ref[k : k + 1, :] == line // 2
        named = jnp.where(match, 1.0, named)
        weighted = jnp.where(
            match, scale_ref[k : k + 1, :].astype(jnp.float32) / 65536.0, weighted
        )
    square = (rows, rows)
    ahead = lax.broadcasted_iota(jnp.int32, square, 0) < lax.broadcasted_iota(
        jnp.int32, square, 1
    )
    before = jnp.dot(
        named, ahead.astype(jnp.float32), preferred_element_type=jnp.float32
    ).astype(jnp.int32)
    kept = before == line % 2
    combine_ref[...] = jnp.where(kept, weighted, 0.0)
    pick = jnp.where(kept, named, 0.0).astype(jnp.bfloat16)

    summed = jnp.sum(parts_ref[...].astype(jnp.float32), axis=0)
    hidden = (share_ref[...].astype(jnp.float32) + summed).astype(jnp.bfloat16)
    hidden_ref[...] = hidden
    wide = hidden.astype(jnp.float32)
    squares = jnp.sum(wide * wide, axis=1, keepdims=True)
    high = squares.astype(jnp.bfloat16).astype(jnp.float32)
    rest = (rows, row_ref.shape[1] - share_width)
    lane = lax.broadcasted_iota(jnp.int32, rest, 1)
    row_ref[:, :share_width] = (wide * gain_here_ref[...]).astype(jnp.bfloat16)
    row_ref[:, share_width:] = jnp.where(
        lane == 0, high, jnp.where(lane == 1, squares - high, 0.0)
    ).astype(jnp.bfloat16)
    out_ref[...] = jnp.dot(
        pick, row_ref[...], preferred_element_type=jnp.float32
    ).astype(jnp.bfloat16)


def swap_rows(rows, outer, inner):
    count = rows.shape[0]
    to = lax.broadcasted_iota(jnp.int32, (count, count), 0)
    at = lax.broadcasted_iota(jnp.int32, (count, count), 1)
    source = ((to // 2) % outer) * (2 * inner) + (to // (2 * outer)) * 2 + to % 2
    return jnp.dot(
        (at == source).astype(jnp.bfloat16), rows, preferred_element_type=jnp.float32
    ).astype(jnp.bfloat16)


def spread_kernel(got_ref, out_ref):
    rows = swap_rows(got_ref[...], GRID[0], GRID[1])
    for y in range(out_ref.shape[0]):
        out_ref[y] = rows


def gather_kernel(parts_ref, out_ref):
    z_size, x_size = GRID[0], GRID[1]
    share = out_ref.shape[1]
    summed = jnp.sum(parts_ref[...].astype(jnp.float32), axis=0)[:, :share]
    out_ref[...] = swap_rows(summed.astype(jnp.bfloat16), x_size, z_size)


def relay_kernel(up_ref, down_hbm, up_out, down_out, down_ref, sem):
    copy = pltpu.make_async_copy(down_hbm, down_ref, sem)
    copy.start()
    y_size = GRID[2]
    share = down_ref.shape[1] // (2 * y_size)
    lanes = down_out.shape[1] // y_size
    up = up_ref[...]
    rest = jnp.zeros((up.shape[0], lanes - share), jnp.bfloat16)
    for y in range(y_size):
        for c in range(2):
            start = (2 * y + c) * share
            up_out[c, :, y * lanes : y * lanes + share] = up[:, start : start + share]
            up_out[c, :, y * lanes + share : (y + 1) * lanes] = rest
    copy.wait()
    for c in range(2):

        @pl.when(lax.axis_index("core") == c)
        def _(c=c):
            for y in range(y_size):
                start = (2 * y + 1 - c) * share
                down_out[:, y * lanes : y * lanes + share] = down_ref[:, start : start + share]
                down_out[:, y * lanes + share : (y + 1) * lanes] = jnp.zeros(
                    (down_ref.shape[0], lanes - share), jnp.bfloat16
                )


def joined(ref):
    return jnp.concatenate([ref[y] for y in range(ref.shape[0])], axis=1)


def expert_kernel(mine_ref, theirs_ref, up_ref, down_ref, act_ref, send_ref, held_ref):
    core = lax.axis_index("core")
    y_size, slots, lanes = mine_ref.shape
    share = FEATURES // (2 * y_size)
    units = act_ref.shape[0]
    projected = jnp.zeros(held_ref.shape, jnp.float32)
    squares = jnp.zeros((slots, 128), jnp.float32)
    for ref, index in ((mine_ref, core), (theirs_ref, 1 - core)):
        projected = projected + lax.dot_general(
            up_ref[index], joined(ref), (((1,), (1,)), ((), ())), preferred_element_type=jnp.float32
        )
        for y in range(y_size):
            squares = squares + ref[y, :, lanes - 128 :].astype(jnp.float32)
    place = lax.broadcasted_iota(jnp.int32, squares.shape, 1) + (lanes - 128 - share)
    squares = jnp.where((place == 0) | (place == 1), squares, 0.0)
    mean_square = jnp.sum(jnp.transpose(squares), axis=0, keepdims=True) / FEATURES
    held_ref[...] = projected * lax.rsqrt(mean_square + epsilon)
    gate = held_ref[pl.ds(0, units, stride=2), :]
    up = held_ref[pl.ds(1, units, stride=2), :]
    act = ((up + 1.0) * gate * jax.nn.sigmoid(swish_alpha * gate)).astype(jnp.bfloat16)
    act_ref[...] = act
    partial = lax.dot_general(
        act, down_ref[...], (((0,), (0,)), ((), ())), preferred_element_type=jnp.float32
    ).astype(jnp.bfloat16)
    for y in range(y_size):
        send_ref[y] = partial[:, y * lanes : (y + 1) * lanes]


def own_kernel(act_ref, down_ref, combine_ref, out_ref, halves_ref):
    y_size = out_ref.shape[0]
    combine = jnp.transpose(combine_ref[...])
    rows = combine.shape[0]
    high = combine.astype(jnp.bfloat16)
    halves_ref[:rows] = high
    halves_ref[rows:] = (combine - high.astype(jnp.float32)).astype(jnp.bfloat16)
    share = down_ref.shape[1] // (2 * y_size)
    partial = lax.dot_general(
        act_ref[...], down_ref[...], (((0,), (0,)), ((), ())), preferred_element_type=jnp.float32
    )
    for c in range(2):

        @pl.when(lax.axis_index("core") == c)
        def _(c=c):
            for y in range(y_size):
                start = (2 * y + c) * share
                out_ref[y, :, :share] = partial[:, start : start + share]


def finish_kernel(hidden_ref, halves_ref, back_ref, out_ref):
    rows = hidden_ref.shape[0]
    mixed = jnp.dot(halves_ref[...], back_ref[...], preferred_element_type=jnp.float32)
    mixture = mixed[:rows] + mixed[rows:]
    out_ref[...] = (hidden_ref[...].astype(jnp.float32) + mixture).astype(jnp.bfloat16)


def run(kernel, name, outs, scratch=(), from_hbm=()):
    vmem = pl.BlockSpec(memory_space=pltpu.VMEM)
    hbm = pl.BlockSpec(memory_space=pltpu.HBM)

    def call(*operands):
        return pl.pallas_call(
            kernel,
            out_shape=tuple(pltpu.VMEM(shape, dtype) for shape, dtype in outs),
            in_specs=[hbm if i in from_hbm else vmem for i in range(len(operands))],
            out_specs=(vmem,) * len(outs),
            scratch_shapes=list(scratch),
            compiler_params=pltpu.CompilerParams(vmem_limit_bytes=16 * MIB),
            name=name,
        )(*operands)

    return call


def local(
    residual,
    queries,
    kv_cache,
    new_kv,
    positions,
    sink_logits,
    out_proj,
    norm_gain,
    route_ids,
    route_weights,
    w_gate_up,
    w_down,
):
    rows, features = residual.shape
    z_size, x_size, y_size, _ = GRID
    share = features // (2 * y_size)
    lanes = pl.cdiv(share, 128) * 128
    slots = 2 * z_size * x_size
    units = w_down.shape[1]
    bf16 = jnp.bfloat16
    swap = [(0, 1), (1, 0)]

    parts = attend(positions, sink_logits, queries, kv_cache, new_kv, out_proj)
    parts = lax.all_to_all(parts, HEAD, 0, 0, tiled=True)
    gate_up = jnp.swapaxes(w_gate_up[0], 0, 1)
    hidden, outgoing, combine = run(
        dispatch_kernel,
        "dispatch",
        [((rows, share), bf16), ((slots, lanes), bf16), ((slots, rows), jnp.float32)],
        [
            pltpu.VMEM((rows, share), bf16),
            pltpu.VMEM((1, share), jnp.float32),
            pltpu.VMEM((rows, lanes), bf16),
        ],
        from_hbm=(5,),
    )(
        parts,
        route_ids.T,
        route_weights.T,
        residual,
        norm_gain,
        pltpu.with_memory_space_constraint(gate_up, pltpu.HBM),
    )

    got = lax.all_to_all(outgoing.reshape(z_size, 2 * x_size, lanes), "z", 0, 0, tiled=True)
    (spread,) = run(spread_kernel, "spread", [((y_size, slots, lanes), bf16)])(
        got.reshape(slots, lanes)
    )
    mine = lax.all_to_all(
        spread.reshape(y_size * x_size, 2 * z_size, lanes), PLANE, 0, 0, tiled=True
    ).reshape(y_size, slots, lanes)
    gate_up, down, mine = lax.optimization_barrier((gate_up, w_down[0], mine))
    gate_up, sent_down = run(
        relay_kernel,
        "relay",
        [((2, 2 * units, y_size * lanes), bf16), ((units, y_size * lanes), bf16)],
        [pltpu.VMEM((units, features), bf16), pltpu.SemaphoreType.DMA],
        from_hbm=(1,),
    )(gate_up, pltpu.with_memory_space_constraint(down, pltpu.HBM))
    theirs = lax.ppermute(mine, "core", swap)
    act, sent = run(
        expert_kernel,
        "expert",
        [((units, slots), bf16), ((y_size, slots, lanes), bf16)],
        [pltpu.VMEM((2 * units, slots), jnp.float32)],
    )(mine, theirs, gate_up, sent_down)

    arrived = lax.ppermute(sent, "core", swap)
    own, halves = run(
        own_kernel,
        "own",
        [((y_size, slots, lanes), jnp.float32), ((2 * rows, slots), bf16)],
    )(act, down, combine)
    paired = (own + arrived.astype(jnp.float32)).astype(bf16)
    paired = lax.all_to_all(
        paired.reshape(y_size * x_size, 2 * z_size, lanes), PLANE, 0, 0, tiled=True
    )
    (summed,) = run(gather_kernel, "gather", [((slots, share), bf16)])(
        paired.reshape(y_size, slots, lanes)
    )
    back = lax.all_to_all(summed.reshape(z_size, 2 * x_size, share), "z", 0, 0, tiled=True)
    return pl.pallas_call(
        finish_kernel,
        out_shape=jax.ShapeDtypeStruct((rows, share), bf16),
        in_specs=[pl.BlockSpec(memory_space=pltpu.VMEM)] * 3,
        out_specs=pl.BlockSpec(memory_space=pltpu.VMEM),
        compiler_params=pltpu.CompilerParams(vmem_limit_bytes=16 * MIB),
        name="finish",
    )(hidden, halves, back.reshape(slots, share))


def solution(mesh):
    fine = Mesh(mesh.devices.reshape(GRID), ("z", "x", "y", "core"))
    in_specs = (
        P(GRP, None),
        P(GRP, HEAD, None),
        P(GRP, HEAD, None, None),
        P(GRP, HEAD, None),
        P(GRP),
        P(HEAD, None),
        P(HEAD, None, None),
        P(),
        P(GRP, None),
        P(GRP, None),
        P(GRP, None, HEAD),
        P(GRP, HEAD, None),
    )
    return jax.shard_map(
        local, mesh=fine, in_specs=in_specs, out_specs=P(GRP, HEAD), check_vma=False
    )
```

```python
import jax
import jax.numpy as jnp
from jax import lax
from jax.experimental import pallas as pl
from jax.experimental.pallas import tpu as pltpu
from jax.sharding import Mesh, PartitionSpec as P


epsilon = 1e-05
swish_alpha = 1.702

GRID = (16, 4, 4, 2)
GRP = ("z", "x")
HEAD = ("y", "core")
PLANE = ("y", "x")
FEATURES = 2880
DOWN_AT = 368
MIB = 1 << 20


def attend_kernel(
    pos_hbm,
    sink_hbm,
    q_hbm,
    kv_hbm,
    new_hbm,
    proj_hbm,
    out_ref,
    pos_ref,
    sink_ref,
    q_ref,
    kv_ref,
    new_ref,
    proj_ref,
    sems,
):
    rows, window, width = kv_ref.shape
    shares = out_ref.shape[0]
    q_copy, kv_copy, new_copy, pos_copy, sink_copy, proj_copy = (
        pltpu.make_async_copy(src, dst, sems.at[i])
        for i, (src, dst) in enumerate(
            [
                (q_hbm, q_ref),
                (kv_hbm, kv_ref),
                (new_hbm, new_ref),
                (pos_hbm, pos_ref),
                (sink_hbm, sink_ref),
                (proj_hbm, proj_ref),
            ]
        )
    )
    for copy in (q_copy, kv_copy, new_copy, pos_copy, sink_copy, proj_copy):
        copy.start()
    half = width // 2
    groups = 4
    share_width = out_ref.shape[2]
    lane = lax.broadcasted_iota(jnp.int32, (rows, width), 1)
    low = lane < half
    q_copy.wait()
    q = q_ref[...].astype(jnp.float32)
    parts = []
    for pair in range(groups // 2):
        both = q[:, pair * width : (pair + 1) * width]
        parts.append(jnp.where(low, both, 0.0))
        parts.append(jnp.where(low, pltpu.roll(both, half, 1), 0.0))
    stacked = jnp.concatenate(parts, axis=0)
    stacked_low = stacked.astype(jnp.bfloat16)
    shape = (groups * rows, window)
    lanes = lax.broadcasted_iota(jnp.int32, shape, 1)
    request = lax.broadcasted_iota(jnp.int32, shape, 0) % rows

    kv_copy.wait()
    kv = kv_ref[...].reshape(rows * window, width)
    found = lax.dot_general(
        stacked_low, kv, (((1,), (1,)), ((), ())), preferred_element_type=jnp.float32
    )
    scores = jnp.zeros(shape, jnp.float32)
    for t in range(rows):
        scores = jnp.where(request == t, found[:, t * window : (t + 1) * window], scores)
    for copy in (new_copy, pos_copy, sink_copy):
        copy.wait()
    new = new_ref[...].astype(jnp.float32)
    new_all = jnp.concatenate([new] * groups, axis=0)
    square = (rows, rows)
    diagonal = lax.broadcasted_iota(jnp.int32, square, 0) == lax.broadcasted_iota(
        jnp.int32, square, 1
    )
    pos = jnp.sum(jnp.where(diagonal, pos_ref[...], 0), axis=1, keepdims=True)
    pos = jnp.concatenate([jnp.broadcast_to(pos, (rows, width))] * groups, axis=0)
    heads = (groups * rows, groups)
    of_head = lax.broadcasted_iota(jnp.int32, heads, 0) // rows == lax.broadcasted_iota(
        jnp.int32, heads, 1
    )
    sink = jnp.sum(jnp.where(of_head, sink_ref[...], 0.0), axis=1, keepdims=True)
    newest = jnp.sum(stacked * new_all, axis=1, keepdims=True)
    is_new = lanes == (pos & (window - 1))
    scores = jnp.where(is_new, newest, scores) * (half**-0.5)
    scores = jnp.where(lanes <= pos, scores, -jnp.inf)
    largest = jnp.maximum(jnp.max(scores, axis=1, keepdims=True), sink)
    raised = jnp.exp(scores - largest)
    total = jnp.sum(raised, axis=1, keepdims=True) + jnp.exp(sink - largest)
    weights = (raised / total).astype(jnp.bfloat16).astype(jnp.float32)
    newest_weight = jnp.sum(jnp.where(is_new, weights, 0.0), axis=1, keepdims=True)
    older = jnp.where(is_new, 0.0, weights)
    spread = jnp.concatenate(
        [jnp.where(request == t, older, 0.0).astype(jnp.bfloat16) for t in range(rows)], axis=1
    )
    mixed = jnp.dot(spread, kv, preferred_element_type=jnp.float32)
    mixed = mixed + newest_weight * new_all
    merged = []
    for pair in range(groups // 2):
        even = mixed[2 * pair * rows : (2 * pair + 1) * rows]
        odd = mixed[(2 * pair + 1) * rows : (2 * pair + 2) * rows]
        merged.append(jnp.where(low, pltpu.roll(even, half, 1), odd))
    merged = jnp.concatenate(merged, axis=1).astype(jnp.bfloat16)
    proj_copy.wait()
    for s in range(shares):
        out_ref[s] = lax.dot_general(
            merged,
            proj_ref[pl.ds(s * share_width, share_width), :],
            (((1,), (1,)), ((), ())),
            preferred_element_type=jnp.float32,
        ).astype(jnp.bfloat16)


def attend(positions, sink_logits, queries, kv_cache, new_kv, out_proj):
    rows, _, window, width = kv_cache.shape
    features = out_proj.shape[2]
    hbm = pl.BlockSpec(memory_space=pltpu.HBM)
    return pl.pallas_call(
        attend_kernel,
        out_shape=pltpu.VMEM((8, rows, features // 8), jnp.bfloat16),
        in_specs=[hbm] * 6,
        out_specs=pl.BlockSpec(memory_space=pltpu.VMEM),
        scratch_shapes=[
            pltpu.VMEM((1, rows), jnp.int32),
            pltpu.VMEM(sink_logits.shape, jnp.float32),
            pltpu.VMEM((rows, queries.shape[2]), jnp.bfloat16),
            pltpu.VMEM((rows, window, width), jnp.bfloat16),
            pltpu.VMEM((rows, width), jnp.bfloat16),
            pltpu.VMEM((features, out_proj.shape[1]), jnp.bfloat16),
            pltpu.SemaphoreType.DMA((6,)),
        ],
        compiler_params=pltpu.CompilerParams(vmem_limit_bytes=16 * MIB),
        name="attend",
    )(
        *(
            pltpu.with_memory_space_constraint(x, pltpu.HBM)
            for x in (
                positions.reshape(1, rows),
                sink_logits,
                queries.reshape(rows, -1),
                kv_cache.reshape(rows, window, width),
                new_kv.reshape(rows, width),
                jnp.swapaxes(out_proj[0], 0, 1),
            )
        )
    )


def dispatch_kernel(
    parts_ref,
    ids_ref,
    scale_ref,
    resid_ref,
    gain_ref,
    later_hbm,
    hidden_ref,
    out_ref,
    combine_ref,
    share_ref,
    gain_here_ref,
    row_ref,
):
    rows, share_width = hidden_ref.shape
    gain = gain_ref[...][None, :]
    here = 2 * lax.axis_index("y") + lax.axis_index("core")
    for s in range(parts_ref.shape[0]):

        @pl.when(here == s)
        def _(s=s):
            share_ref[...] = resid_ref[:, s * share_width : (s + 1) * share_width]
            gain_here_ref[...] = gain[:, s * share_width : (s + 1) * share_width]

    line = lax.broadcasted_iota(jnp.int32, combine_ref.shape, 0)
    named = jnp.zeros(combine_ref.shape, jnp.float32)
    weighted = jnp.zeros(combine_ref.shape, jnp.float32)
    for k in range(ids_ref.shape[0]):
        match = ids_ref[k : k + 1, :] == line // 2
        named = jnp.where(match, 1.0, named)
        weighted = jnp.where(
            match, scale_ref[k : k + 1, :].astype(jnp.float32) / 65536.0, weighted
        )
    square = (rows, rows)
    ahead = lax.broadcasted_iota(jnp.int32, square, 0) < lax.broadcasted_iota(
        jnp.int32, square, 1
    )
    before = jnp.dot(
        named, ahead.astype(jnp.float32), preferred_element_type=jnp.float32
    ).astype(jnp.int32)
    kept = before == line % 2
    combine_ref[...] = jnp.where(kept, weighted, 0.0)
    pick = jnp.where(kept, named, 0.0).astype(jnp.bfloat16)

    summed = jnp.sum(parts_ref[...].astype(jnp.float32), axis=0)
    hidden = (share_ref[...].astype(jnp.float32) + summed).astype(jnp.bfloat16)
    hidden_ref[...] = hidden
    wide = hidden.astype(jnp.float32)
    squares = jnp.sum(wide * wide, axis=1, keepdims=True)
    high = squares.astype(jnp.bfloat16).astype(jnp.float32)
    rest = (rows, row_ref.shape[1] - share_width)
    lane = lax.broadcasted_iota(jnp.int32, rest, 1)
    row_ref[:, :share_width] = (wide * gain_here_ref[...]).astype(jnp.bfloat16)
    row_ref[:, share_width:] = jnp.where(
        lane == 0, high, jnp.where(lane == 1, squares - high, 0.0)
    ).astype(jnp.bfloat16)
    out_ref[...] = jnp.dot(
        pick, row_ref[...], preferred_element_type=jnp.float32
    ).astype(jnp.bfloat16)


def swap_rows(rows, outer, inner):
    count = rows.shape[0]
    to = lax.broadcasted_iota(jnp.int32, (count, count), 0)
    at = lax.broadcasted_iota(jnp.int32, (count, count), 1)
    source = ((to // 2) % outer) * (2 * inner) + (to // (2 * outer)) * 2 + to % 2
    return jnp.dot(
        (at == source).astype(jnp.bfloat16), rows, preferred_element_type=jnp.float32
    ).astype(jnp.bfloat16)


def spread_kernel(got_ref, out_ref):
    rows = swap_rows(got_ref[...], GRID[0], GRID[1])
    for y in range(out_ref.shape[0]):
        out_ref[y] = rows


def gather_kernel(parts_ref, out_ref):
    z_size, x_size = GRID[0], GRID[1]
    share = out_ref.shape[1]
    summed = jnp.sum(parts_ref[...].astype(jnp.float32), axis=0)[:, :share]
    out_ref[...] = swap_rows(summed.astype(jnp.bfloat16), x_size, z_size)


def lay(source, out, first, c):
    y_size = GRID[2]
    share = source.shape[1] // (2 * y_size)
    lanes = out.shape[1] // y_size
    count = source.shape[0]
    at = pl.ds(first, count)
    for y in range(y_size):
        start = (2 * y + c) * share
        out[at, y * lanes : y * lanes + share] = source[:, start : start + share]
        out[at, y * lanes + share : (y + 1) * lanes] = jnp.zeros(
            (count, lanes - share), jnp.bfloat16
        )


def for_core(act):
    for c in range(2):

        @pl.when(lax.axis_index("core") == c)
        def _(c=c):
            act(c)


def relay_kernel(
    up_ref, down_hbm, combine_ref, up_out, send_hbm, halves_ref, send_ref, down_ref, sems
):
    copy = pltpu.make_async_copy(down_hbm, down_ref, sems.at[0])
    copy.start()
    for_core(lambda c: lay(up_ref[...], send_ref, 0, 1 - c))
    top = pltpu.make_async_copy(
        send_ref.at[pl.ds(0, DOWN_AT)], send_hbm.at[pl.ds(0, DOWN_AT)], sems.at[1]
    )
    top.start()
    for_core(lambda c: lay(up_ref[...], up_out, 0, c))
    combine = jnp.transpose(combine_ref[...])
    rows = combine.shape[0]
    high = combine.astype(jnp.bfloat16)
    halves_ref[:rows] = high
    halves_ref[rows:] = (combine - high.astype(jnp.float32)).astype(jnp.bfloat16)
    copy.wait()
    for_core(lambda c: lay(down_ref[...], send_ref, DOWN_AT, 1 - c))
    rest = send_ref.shape[0] - DOWN_AT
    bottom = pltpu.make_async_copy(
        send_ref.at[pl.ds(DOWN_AT, rest)], send_hbm.at[pl.ds(DOWN_AT, rest)], sems.at[2]
    )
    bottom.start()
    top.wait()
    bottom.wait()


def keep_kernel(down_hbm, after_ref, out_ref, down_ref, sem):
    copy = pltpu.make_async_copy(down_hbm, down_ref, sem)
    copy.start()
    copy.wait()
    for_core(lambda c: lay(down_ref[...], out_ref, 0, c))


def joined(ref):
    return jnp.concatenate([ref[y] for y in range(ref.shape[0])], axis=1)


def project_kernel(mine_ref, up_ref, partner_ref, out_ref):
    y_size, slots, lanes = mine_ref.shape
    share = FEATURES // (2 * y_size)
    columns = up_ref.shape[0]
    x = joined(mine_ref)
    for block, ref in enumerate((up_ref, partner_ref)):
        out_ref[pl.ds(block * columns, columns), :] = lax.dot_general(
            ref[pl.ds(0, columns), :],
            x,
            (((1,), (1,)), ((), ())),
            preferred_element_type=jnp.float32,
        )
    squares = jnp.zeros((slots, 128), jnp.float32)
    for y in range(y_size):
        squares = squares + mine_ref[y, :, lanes - 128 :].astype(jnp.float32)
    place = lax.broadcasted_iota(jnp.int32, squares.shape, 1) + (lanes - 128 - share)
    squares = jnp.where((place == 0) | (place == 1), squares, 0.0)
    squares = jnp.sum(jnp.transpose(squares), axis=0, keepdims=True)
    tail = out_ref.shape[0] - 2 * columns
    out_ref[pl.ds(2 * columns, tail), :] = jnp.broadcast_to(squares, (tail, slots))


def down_kernel(here_ref, there_ref, down_ref, partner_ref, out_ref, held_ref):
    units = down_ref.shape[0]
    columns = 2 * units
    y_size, _, lanes = out_ref.shape
    last = here_ref.shape[0] - 1
    squares = here_ref[last : last + 1, :] + there_ref[last : last + 1, :]
    scale = lax.rsqrt(squares / FEATURES + epsilon)
    total = jnp.zeros((out_ref.shape[1], y_size * lanes), jnp.float32)
    for block, weights in enumerate((down_ref[...], partner_ref[pl.ds(DOWN_AT, units), :])):
        held_ref[block] = (
            here_ref[pl.ds(block * columns, columns), :]
            + there_ref[pl.ds((1 - block) * columns, columns), :]
        ) * scale
        gate = held_ref[block, pl.ds(0, units, stride=2), :]
        up = held_ref[block, pl.ds(1, units, stride=2), :]
        act = ((up + 1.0) * gate * jax.nn.sigmoid(swish_alpha * gate)).astype(jnp.bfloat16)
        total = total + lax.dot_general(
            act, weights, (((0,), (0,)), ((), ())), preferred_element_type=jnp.float32
        )
    for y in range(y_size):
        out_ref[y] = total[:, y * lanes : (y + 1) * lanes].astype(jnp.bfloat16)


def finish_kernel(hidden_ref, halves_ref, back_ref, out_ref):
    rows = hidden_ref.shape[0]
    mixed = jnp.dot(halves_ref[...], back_ref[...], preferred_element_type=jnp.float32)
    mixture = mixed[:rows] + mixed[rows:]
    out_ref[...] = (hidden_ref[...].astype(jnp.float32) + mixture).astype(jnp.bfloat16)


def run(kernel, outs, scratch=(), from_hbm=()):
    vmem = pl.BlockSpec(memory_space=pltpu.VMEM)
    hbm = pl.BlockSpec(memory_space=pltpu.HBM)

    def call(*operands):
        return pl.pallas_call(
            kernel,
            out_shape=tuple(pltpu.VMEM(shape, dtype) for shape, dtype in outs),
            in_specs=[hbm if i in from_hbm else vmem for i in range(len(operands))],
            out_specs=(vmem,) * len(outs),
            scratch_shapes=list(scratch),
            compiler_params=pltpu.CompilerParams(vmem_limit_bytes=16 * MIB),
        )(*operands)

    return call


def local(
    residual,
    queries,
    kv_cache,
    new_kv,
    positions,
    sink_logits,
    out_proj,
    norm_gain,
    route_ids,
    route_weights,
    w_gate_up,
    w_down,
):
    rows, features = residual.shape
    z_size, x_size, y_size, _ = GRID
    share = features // (2 * y_size)
    lanes = pl.cdiv(share, 128) * 128
    slots = 2 * z_size * x_size
    units = w_down.shape[1]
    bf16 = jnp.bfloat16
    swap = [(0, 1), (1, 0)]

    parts = attend(positions, sink_logits, queries, kv_cache, new_kv, out_proj)
    parts = lax.all_to_all(parts, HEAD, 0, 0, tiled=True)
    gate_up = jnp.swapaxes(w_gate_up[0], 0, 1)
    hidden, outgoing, combine = run(
        dispatch_kernel,
        [((rows, share), bf16), ((slots, lanes), bf16), ((slots, rows), jnp.float32)],
        [
            pltpu.VMEM((rows, share), bf16),
            pltpu.VMEM((1, share), jnp.float32),
            pltpu.VMEM((rows, lanes), bf16),
        ],
        from_hbm=(5,),
    )(
        parts,
        route_ids.T,
        route_weights.T,
        residual,
        norm_gain,
        pltpu.with_memory_space_constraint(gate_up, pltpu.HBM),
    )

    outgoing, gate_up, down = lax.optimization_barrier((outgoing, gate_up, w_down[0]))
    down = pltpu.with_memory_space_constraint(down, pltpu.HBM)
    width = y_size * lanes
    sent_rows = DOWN_AT + pl.cdiv(units, 16) * 16
    vmem = pl.BlockSpec(memory_space=pltpu.VMEM)
    hbm = pl.BlockSpec(memory_space=pltpu.HBM)
    gate_up, to_partner, halves = pl.pallas_call(
        relay_kernel,
        out_shape=(
            pltpu.VMEM((2 * units, width), bf16),
            pltpu.HBM((sent_rows, width), bf16),
            pltpu.VMEM((2 * rows, slots), bf16),
        ),
        in_specs=[vmem, hbm, vmem],
        out_specs=(vmem, hbm, vmem),
        scratch_shapes=[
            pltpu.VMEM((sent_rows, width), bf16),
            pltpu.VMEM((units, features), bf16),
            pltpu.SemaphoreType.DMA((3,)),
        ],
        compiler_params=pltpu.CompilerParams(vmem_limit_bytes=16 * MIB),
        name="relay",
    )(gate_up, down, combine)
    partner = lax.ppermute(to_partner, "core", swap)

    got = lax.all_to_all(outgoing.reshape(z_size, 2 * x_size, lanes), "z", 0, 0, tiled=True)
    got, gate_up, halves = lax.optimization_barrier((got, gate_up, halves))
    (spread,) = run(spread_kernel, [((y_size, slots, lanes), bf16)])(got.reshape(slots, lanes))
    mine = lax.all_to_all(
        spread.reshape(y_size * x_size, 2 * z_size, lanes), PLANE, 0, 0, tiled=True
    ).reshape(y_size, slots, lanes)

    (projected,) = run(project_kernel, [((4 * units + 8, slots), jnp.float32)])(
        mine, gate_up, partner
    )
    (kept_down,) = run(
        keep_kernel,
        [((units, width), bf16)],
        [pltpu.VMEM((units, features), bf16), pltpu.SemaphoreType.DMA],
        from_hbm=(0,),
    )(down, projected)
    theirs = lax.ppermute(projected, "core", swap)
    (paired,) = run(
        down_kernel,
        [((y_size, slots, lanes), bf16)],
        [pltpu.VMEM((2, 2 * units, slots), jnp.float32)],
    )(projected, theirs, kept_down, partner)

    paired = lax.all_to_all(
        paired.reshape(y_size * x_size, 2 * z_size, lanes), PLANE, 0, 0, tiled=True
    )
    (summed,) = run(gather_kernel, [((slots, share), bf16)])(paired.reshape(y_size, slots, lanes))
    back = lax.all_to_all(summed.reshape(z_size, 2 * x_size, share), "z", 0, 0, tiled=True)
    return pl.pallas_call(
        finish_kernel,
        out_shape=jax.ShapeDtypeStruct((rows, share), bf16),
        in_specs=[pl.BlockSpec(memory_space=pltpu.VMEM)] * 3,
        out_specs=pl.BlockSpec(memory_space=pltpu.VMEM),
        compiler_params=pltpu.CompilerParams(vmem_limit_bytes=16 * MIB),
        name="finish",
    )(hidden, halves, back.reshape(slots, share))


def solution(mesh):
    fine = Mesh(mesh.devices.reshape(GRID), ("z", "x", "y", "core"))
    in_specs = (
        P(GRP, None),
        P(GRP, HEAD, None),
        P(GRP, HEAD, None, None),
        P(GRP, HEAD, None),
        P(GRP),
        P(HEAD, None),
        P(HEAD, None, None),
        P(),
        P(GRP, None),
        P(GRP, None),
        P(GRP, None, HEAD),
        P(GRP, HEAD, None),
    )
    return jax.shard_map(
        local, mesh=fine, in_specs=in_specs, out_specs=P(GRP, HEAD), check_vma=False
    )
```

```python
import jax
import jax.numpy as jnp
from jax import lax
from jax.experimental import pallas as pl
from jax.experimental.pallas import tpu as pltpu
from jax.sharding import Mesh, PartitionSpec as P


epsilon = 1e-05
swish_alpha = 1.702

GRID = (16, 4, 4, 2)
GRP = ("z", "x")
HEAD = ("y", "core")
PLANE = ("y", "x")
FEATURES = 2880
DOWN_AT = 368
MIB = 1 << 20


def attend_kernel(
    pos_hbm,
    sink_hbm,
    q_hbm,
    kv_hbm,
    new_hbm,
    proj_hbm,
    out_ref,
    pos_ref,
    sink_ref,
    q_ref,
    kv_ref,
    new_ref,
    proj_ref,
    sems,
):
    rows, window, width = kv_ref.shape
    shares = out_ref.shape[0]
    q_copy, kv_copy, new_copy, pos_copy, sink_copy, proj_copy = (
        pltpu.make_async_copy(src, dst, sems.at[i])
        for i, (src, dst) in enumerate(
            [
                (q_hbm, q_ref),
                (kv_hbm, kv_ref),
                (new_hbm, new_ref),
                (pos_hbm, pos_ref),
                (sink_hbm, sink_ref),
                (proj_hbm, proj_ref),
            ]
        )
    )
    for copy in (q_copy, kv_copy, new_copy, pos_copy, sink_copy, proj_copy):
        copy.start()
    half = width // 2
    groups = 4
    share_width = out_ref.shape[2]
    lane = lax.broadcasted_iota(jnp.int32, (rows, width), 1)
    low = lane < half
    q_copy.wait()
    q = q_ref[...].astype(jnp.float32)
    parts = []
    for pair in range(groups // 2):
        both = q[:, pair * width : (pair + 1) * width]
        parts.append(jnp.where(low, both, 0.0))
        parts.append(jnp.where(low, pltpu.roll(both, half, 1), 0.0))
    stacked = jnp.concatenate(parts, axis=0)
    stacked_low = stacked.astype(jnp.bfloat16)
    shape = (groups * rows, window)
    lanes = lax.broadcasted_iota(jnp.int32, shape, 1)
    request = lax.broadcasted_iota(jnp.int32, shape, 0) % rows

    kv_copy.wait()
    kv = kv_ref[...].reshape(rows * window, width)
    found = lax.dot_general(
        stacked_low, kv, (((1,), (1,)), ((), ())), preferred_element_type=jnp.float32
    )
    scores = jnp.zeros(shape, jnp.float32)
    for t in range(rows):
        scores = jnp.where(request == t, found[:, t * window : (t + 1) * window], scores)
    for copy in (new_copy, pos_copy, sink_copy):
        copy.wait()
    new = new_ref[...].astype(jnp.float32)
    new_all = jnp.concatenate([new] * groups, axis=0)
    square = (rows, rows)
    diagonal = lax.broadcasted_iota(jnp.int32, square, 0) == lax.broadcasted_iota(
        jnp.int32, square, 1
    )
    pos = jnp.sum(jnp.where(diagonal, pos_ref[...], 0), axis=1, keepdims=True)
    pos = jnp.concatenate([jnp.broadcast_to(pos, (rows, width))] * groups, axis=0)
    heads = (groups * rows, groups)
    of_head = lax.broadcasted_iota(jnp.int32, heads, 0) // rows == lax.broadcasted_iota(
        jnp.int32, heads, 1
    )
    sink = jnp.sum(jnp.where(of_head, sink_ref[...], 0.0), axis=1, keepdims=True)
    newest = jnp.sum(stacked * new_all, axis=1, keepdims=True)
    is_new = lanes == (pos & (window - 1))
    scores = jnp.where(is_new, newest, scores) * (half**-0.5)
    scores = jnp.where(lanes <= pos, scores, -jnp.inf)
    largest = jnp.maximum(jnp.max(scores, axis=1, keepdims=True), sink)
    raised = jnp.exp(scores - largest)
    total = jnp.sum(raised, axis=1, keepdims=True) + jnp.exp(sink - largest)
    weights = (raised / total).astype(jnp.bfloat16).astype(jnp.float32)
    newest_weight = jnp.sum(jnp.where(is_new, weights, 0.0), axis=1, keepdims=True)
    older = jnp.where(is_new, 0.0, weights)
    spread = jnp.concatenate(
        [jnp.where(request == t, older, 0.0).astype(jnp.bfloat16) for t in range(rows)], axis=1
    )
    mixed = jnp.dot(spread, kv, preferred_element_type=jnp.float32)
    mixed = mixed + newest_weight * new_all
    merged = []
    for pair in range(groups // 2):
        even = mixed[2 * pair * rows : (2 * pair + 1) * rows]
        odd = mixed[(2 * pair + 1) * rows : (2 * pair + 2) * rows]
        merged.append(jnp.where(low, pltpu.roll(even, half, 1), odd))
    merged = jnp.concatenate(merged, axis=1).astype(jnp.bfloat16)
    proj_copy.wait()
    for s in range(shares):
        out_ref[(s % 2) * (shares // 2) + s // 2] = lax.dot_general(
            merged,
            proj_ref[pl.ds(s * share_width, share_width), :],
            (((1,), (1,)), ((), ())),
            preferred_element_type=jnp.float32,
        ).astype(jnp.bfloat16)


def attend(positions, sink_logits, queries, kv_cache, new_kv, out_proj):
    rows, _, window, width = kv_cache.shape
    features = out_proj.shape[2]
    hbm = pl.BlockSpec(memory_space=pltpu.HBM)
    return pl.pallas_call(
        attend_kernel,
        out_shape=pltpu.VMEM((8, rows, features // 8), jnp.bfloat16),
        in_specs=[hbm] * 6,
        out_specs=pl.BlockSpec(memory_space=pltpu.VMEM),
        scratch_shapes=[
            pltpu.VMEM((1, rows), jnp.int32),
            pltpu.VMEM(sink_logits.shape, jnp.float32),
            pltpu.VMEM((rows, queries.shape[2]), jnp.bfloat16),
            pltpu.VMEM((rows, window, width), jnp.bfloat16),
            pltpu.VMEM((rows, width), jnp.bfloat16),
            pltpu.VMEM((features, out_proj.shape[1]), jnp.bfloat16),
            pltpu.SemaphoreType.DMA((6,)),
        ],
        compiler_params=pltpu.CompilerParams(vmem_limit_bytes=16 * MIB),
        name="attend",
    )(
        *(
            pltpu.with_memory_space_constraint(x, pltpu.HBM)
            for x in (
                positions.reshape(1, rows),
                sink_logits,
                queries.reshape(rows, -1),
                kv_cache.reshape(rows, window, width),
                new_kv.reshape(rows, width),
                jnp.swapaxes(out_proj[0], 0, 1),
            )
        )
    )


def dispatch_kernel(
    parts_ref,
    ids_ref,
    scale_ref,
    resid_ref,
    gain_ref,
    later_hbm,
    hidden_ref,
    out_ref,
    combine_ref,
    share_ref,
    gain_here_ref,
    row_ref,
):
    rows, share_width = hidden_ref.shape
    gain = gain_ref[...][None, :]
    here = 2 * lax.axis_index("y") + lax.axis_index("core")
    for s in range(parts_ref.shape[0]):

        @pl.when(here == s)
        def _(s=s):
            share_ref[...] = resid_ref[:, s * share_width : (s + 1) * share_width]
            gain_here_ref[...] = gain[:, s * share_width : (s + 1) * share_width]

    line = lax.broadcasted_iota(jnp.int32, combine_ref.shape, 0)
    named = jnp.zeros(combine_ref.shape, jnp.float32)
    weighted = jnp.zeros(combine_ref.shape, jnp.float32)
    for k in range(ids_ref.shape[0]):
        match = ids_ref[k : k + 1, :] == line // 2
        named = jnp.where(match, 1.0, named)
        weighted = jnp.where(
            match, scale_ref[k : k + 1, :].astype(jnp.float32) / 65536.0, weighted
        )
    square = (rows, rows)
    ahead = lax.broadcasted_iota(jnp.int32, square, 0) < lax.broadcasted_iota(
        jnp.int32, square, 1
    )
    before = jnp.dot(
        named, ahead.astype(jnp.float32), preferred_element_type=jnp.float32
    ).astype(jnp.int32)
    kept = before == line % 2
    combine_ref[...] = jnp.where(kept, weighted, 0.0)
    pick = jnp.where(kept, named, 0.0).astype(jnp.bfloat16)

    summed = jnp.sum(parts_ref[...].astype(jnp.float32), axis=0)
    hidden = (share_ref[...].astype(jnp.float32) + summed).astype(jnp.bfloat16)
    hidden_ref[...] = hidden
    wide = hidden.astype(jnp.float32)
    squares = jnp.sum(wide * wide, axis=1, keepdims=True)
    high = squares.astype(jnp.bfloat16).astype(jnp.float32)
    rest = (rows, row_ref.shape[1] - share_width)
    lane = lax.broadcasted_iota(jnp.int32, rest, 1)
    row_ref[:, :share_width] = (wide * gain_here_ref[...]).astype(jnp.bfloat16)
    row_ref[:, share_width:] = jnp.where(
        lane == 0, high, jnp.where(lane == 1, squares - high, 0.0)
    ).astype(jnp.bfloat16)
    out_ref[...] = jnp.dot(
        pick, row_ref[...], preferred_element_type=jnp.float32
    ).astype(jnp.bfloat16)


def swap_rows(rows, outer, inner):
    count = rows.shape[0]
    to = lax.broadcasted_iota(jnp.int32, (count, count), 0)
    at = lax.broadcasted_iota(jnp.int32, (count, count), 1)
    source = ((to // 2) % outer) * (2 * inner) + (to // (2 * outer)) * 2 + to % 2
    return jnp.dot(
        (at == source).astype(jnp.bfloat16), rows, preferred_element_type=jnp.float32
    ).astype(jnp.bfloat16)


def spread_kernel(got_ref, out_ref):
    rows = swap_rows(got_ref[...], GRID[0], GRID[1])
    for y in range(out_ref.shape[0]):
        out_ref[y] = rows


def gather_kernel(parts_ref, out_ref):
    z_size, x_size = GRID[0], GRID[1]
    share = out_ref.shape[1]
    summed = jnp.sum(parts_ref[...].astype(jnp.float32), axis=0)[:, :share]
    out_ref[...] = swap_rows(summed.astype(jnp.bfloat16), x_size, z_size)


def lay(source, out, first, c):
    y_size = GRID[2]
    share = source.shape[1] // (2 * y_size)
    lanes = out.shape[1] // y_size
    count = source.shape[0]
    at = pl.ds(first, count)
    for y in range(y_size):
        start = (2 * y + c) * share
        out[at, y * lanes : y * lanes + share] = source[:, start : start + share]
        out[at, y * lanes + share : (y + 1) * lanes] = jnp.zeros(
            (count, lanes - share), jnp.bfloat16
        )


def for_core(act):
    for c in range(2):

        @pl.when(lax.axis_index("core") == c)
        def _(c=c):
            act(c)


def relay_kernel(
    up_ref, down_hbm, combine_ref, up_out, send_hbm, halves_ref, send_ref, down_ref, sems
):
    copy = pltpu.make_async_copy(down_hbm, down_ref, sems.at[0])
    copy.start()
    for_core(lambda c: lay(up_ref[...], send_ref, 0, 1 - c))
    top = pltpu.make_async_copy(
        send_ref.at[pl.ds(0, DOWN_AT)], send_hbm.at[pl.ds(0, DOWN_AT)], sems.at[1]
    )
    top.start()
    for_core(lambda c: lay(up_ref[...], up_out, 0, c))
    combine = jnp.transpose(combine_ref[...])
    rows = combine.shape[0]
    high = combine.astype(jnp.bfloat16)
    halves_ref[:rows] = high
    halves_ref[rows:] = (combine - high.astype(jnp.float32)).astype(jnp.bfloat16)
    copy.wait()
    for_core(lambda c: lay(down_ref[...], send_ref, DOWN_AT, 1 - c))
    rest = send_ref.shape[0] - DOWN_AT
    bottom = pltpu.make_async_copy(
        send_ref.at[pl.ds(DOWN_AT, rest)], send_hbm.at[pl.ds(DOWN_AT, rest)], sems.at[2]
    )
    bottom.start()
    top.wait()
    bottom.wait()


def keep_kernel(down_ref, after_ref, out_ref):
    for_core(lambda c: lay(down_ref[...], out_ref, 0, c))


def joined(ref):
    return jnp.concatenate([ref[y] for y in range(ref.shape[0])], axis=1)


def project_kernel(mine_ref, up_ref, partner_ref, later_hbm, out_ref, send_ref):
    y_size, slots, lanes = mine_ref.shape
    share = FEATURES // (2 * y_size)
    columns = up_ref.shape[0]
    x = joined(mine_ref)
    for block, ref in enumerate((up_ref, partner_ref)):
        found = lax.dot_general(
            ref[pl.ds(0, columns), :],
            x,
            (((1,), (1,)), ((), ())),
            preferred_element_type=jnp.float32,
        )
        out_ref[pl.ds(block * columns, columns), :] = found
        send_ref[pl.ds(block * columns, columns), :] = found.astype(jnp.bfloat16)
    squares = jnp.zeros((slots, 128), jnp.float32)
    for y in range(y_size):
        squares = squares + mine_ref[y, :, lanes - 128 :].astype(jnp.float32)
    place = lax.broadcasted_iota(jnp.int32, squares.shape, 1) + (lanes - 128 - share)
    squares = jnp.where((place == 0) | (place == 1), squares, 0.0)
    squares = jnp.sum(jnp.transpose(squares), axis=0, keepdims=True)
    tail = out_ref.shape[0] - 2 * columns
    out_ref[pl.ds(2 * columns, tail), :] = jnp.broadcast_to(squares, (tail, slots))
    tail = send_ref.shape[0] - 2 * columns
    high = squares.astype(jnp.bfloat16).astype(jnp.float32)
    first = lax.broadcasted_iota(jnp.int32, (tail, slots), 0) == 0
    send_ref[pl.ds(2 * columns, tail), :] = jnp.where(first, high, squares - high).astype(
        jnp.bfloat16
    )


def down_kernel(here_ref, there_ref, down_ref, partner_ref, out_ref, held_ref):
    units = down_ref.shape[0]
    columns = 2 * units
    y_size, _, lanes = out_ref.shape
    last = here_ref.shape[0] - 1
    tail = there_ref[pl.ds(2 * columns, there_ref.shape[0] - 2 * columns), :].astype(jnp.float32)
    squares = here_ref[last : last + 1, :] + tail[0:1, :] + tail[1:2, :]
    scale = lax.rsqrt(squares / FEATURES + epsilon)
    total = jnp.zeros((out_ref.shape[1], y_size * lanes), jnp.float32)
    for block, weights in enumerate((down_ref[...], partner_ref[pl.ds(DOWN_AT, units), :])):
        theirs = there_ref[pl.ds((1 - block) * columns, columns), :].astype(jnp.float32)
        held_ref[block] = (here_ref[pl.ds(block * columns, columns), :] + theirs) * scale
        gate = held_ref[block, pl.ds(0, units, stride=2), :]
        up = held_ref[block, pl.ds(1, units, stride=2), :]
        act = ((up + 1.0) * gate * jax.nn.sigmoid(swish_alpha * gate)).astype(jnp.bfloat16)
        total = total + lax.dot_general(
            act, weights, (((0,), (0,)), ((), ())), preferred_element_type=jnp.float32
        )
    for y in range(y_size):
        out_ref[y] = total[:, y * lanes : (y + 1) * lanes].astype(jnp.bfloat16)


def finish_kernel(hidden_ref, halves_ref, back_ref, out_ref):
    rows = hidden_ref.shape[0]
    mixed = jnp.dot(halves_ref[...], back_ref[...], preferred_element_type=jnp.float32)
    mixture = mixed[:rows] + mixed[rows:]
    out_ref[...] = (hidden_ref[...].astype(jnp.float32) + mixture).astype(jnp.bfloat16)


def run(kernel, outs, scratch=(), from_hbm=()):
    vmem = pl.BlockSpec(memory_space=pltpu.VMEM)
    hbm = pl.BlockSpec(memory_space=pltpu.HBM)

    def call(*operands):
        return pl.pallas_call(
            kernel,
            out_shape=tuple(pltpu.VMEM(shape, dtype) for shape, dtype in outs),
            in_specs=[hbm if i in from_hbm else vmem for i in range(len(operands))],
            out_specs=(vmem,) * len(outs),
            scratch_shapes=list(scratch),
            compiler_params=pltpu.CompilerParams(vmem_limit_bytes=16 * MIB),
        )(*operands)

    return call


def local(
    residual,
    queries,
    kv_cache,
    new_kv,
    positions,
    sink_logits,
    out_proj,
    norm_gain,
    route_ids,
    route_weights,
    w_gate_up,
    w_down,
):
    rows, features = residual.shape
    z_size, x_size, y_size, _ = GRID
    share = features // (2 * y_size)
    lanes = pl.cdiv(share, 128) * 128
    slots = 2 * z_size * x_size
    units = w_down.shape[1]
    bf16 = jnp.bfloat16
    swap = [(0, 1), (1, 0)]

    parts = attend(positions, sink_logits, queries, kv_cache, new_kv, out_proj)
    parts = lax.all_to_all(parts, ("core", "y"), 0, 0, tiled=True)
    gate_up = jnp.swapaxes(w_gate_up[0], 0, 1)
    hidden, outgoing, combine = run(
        dispatch_kernel,
        [((rows, share), bf16), ((slots, lanes), bf16), ((slots, rows), jnp.float32)],
        [
            pltpu.VMEM((rows, share), bf16),
            pltpu.VMEM((1, share), jnp.float32),
            pltpu.VMEM((rows, lanes), bf16),
        ],
        from_hbm=(5,),
    )(
        parts,
        route_ids.T,
        route_weights.T,
        residual,
        norm_gain,
        pltpu.with_memory_space_constraint(gate_up, pltpu.HBM),
    )

    outgoing, gate_up, down = lax.optimization_barrier((outgoing, gate_up, w_down[0]))
    down = pltpu.with_memory_space_constraint(down, pltpu.HBM)
    width = y_size * lanes
    sent_rows = DOWN_AT + pl.cdiv(units, 16) * 16
    vmem = pl.BlockSpec(memory_space=pltpu.VMEM)
    hbm = pl.BlockSpec(memory_space=pltpu.HBM)
    gate_up, to_partner, halves = pl.pallas_call(
        relay_kernel,
        out_shape=(
            pltpu.VMEM((2 * units, width), bf16),
            pltpu.HBM((sent_rows, width), bf16),
            pltpu.VMEM((2 * rows, slots), bf16),
        ),
        in_specs=[vmem, hbm, vmem],
        out_specs=(vmem, hbm, vmem),
        scratch_shapes=[
            pltpu.VMEM((sent_rows, width), bf16),
            pltpu.VMEM((units, features), bf16),
            pltpu.SemaphoreType.DMA((3,)),
        ],
        compiler_params=pltpu.CompilerParams(vmem_limit_bytes=16 * MIB),
        name="relay",
    )(gate_up, down, combine)
    partner = lax.ppermute(to_partner, "core", swap)

    got = lax.all_to_all(outgoing.reshape(z_size, 2 * x_size, lanes), "z", 0, 0, tiled=True)
    got, gate_up, halves = lax.optimization_barrier((got, gate_up, halves))
    (spread,) = run(spread_kernel, [((y_size, slots, lanes), bf16)])(got.reshape(slots, lanes))
    mine = lax.all_to_all(
        spread.reshape(y_size * x_size, 2 * z_size, lanes), PLANE, 0, 0, tiled=True
    ).reshape(y_size, slots, lanes)

    projected, to_swap = run(
        project_kernel,
        [((4 * units + 8, slots), jnp.float32), ((4 * units + 16, slots), bf16)],
        from_hbm=(3,),
    )(mine, gate_up, partner, pltpu.with_memory_space_constraint(w_down[0], pltpu.HBM))
    (kept_down,) = run(keep_kernel, [((units, width), bf16)])(w_down[0], projected)
    theirs = lax.ppermute(to_swap, "core", swap)
    (paired,) = run(
        down_kernel,
        [((y_size, slots, lanes), bf16)],
        [pltpu.VMEM((2, 2 * units, slots), jnp.float32)],
    )(projected, theirs, kept_down, partner)

    paired = lax.all_to_all(
        paired.reshape(y_size * x_size, 2 * z_size, lanes), PLANE, 0, 0, tiled=True
    )
    (summed,) = run(gather_kernel, [((slots, share), bf16)])(paired.reshape(y_size, slots, lanes))
    back = lax.all_to_all(summed.reshape(z_size, 2 * x_size, share), "z", 0, 0, tiled=True)
    return pl.pallas_call(
        finish_kernel,
        out_shape=jax.ShapeDtypeStruct((rows, share), bf16),
        in_specs=[pl.BlockSpec(memory_space=pltpu.VMEM)] * 3,
        out_specs=pl.BlockSpec(memory_space=pltpu.VMEM),
        compiler_params=pltpu.CompilerParams(vmem_limit_bytes=16 * MIB),
        name="finish",
    )(hidden, halves, back.reshape(slots, share))


def solution(mesh):
    fine = Mesh(mesh.devices.reshape(GRID), ("z", "x", "y", "core"))
    in_specs = (
        P(GRP, None),
        P(GRP, HEAD, None),
        P(GRP, HEAD, None, None),
        P(GRP, HEAD, None),
        P(GRP),
        P(HEAD, None),
        P(HEAD, None, None),
        P(),
        P(GRP, None),
        P(GRP, None),
        P(GRP, None, HEAD),
        P(GRP, HEAD, None),
    )
    return jax.shard_map(
        local, mesh=fine, in_specs=in_specs, out_specs=P(GRP, HEAD), check_vma=False
    )
```
